32 devices in a mesh: dp: 4 (over y, z), tp: 8 (over x, core).
Axes of the slice: x: 4, y: 2, z: 2, core: 2. Of those that a mesh axis runs over, the one named last changes fastest.
The devices are a block of a 4x4x8 slice.
Arguments:
- x: bfloat16 [256, 8192], P('dp'), parts along dimension 0
- ln_attn_gamma: float32 [8192], replicated
- ln_attn_beta: float32 [8192], replicated
- ln_mlp_gamma: float32 [8192], replicated
- ln_mlp_beta: float32 [8192], replicated
- w_qkv: bfloat16 [8192, 8, 18, 64], P(None, 'tp')
- w_out: bfloat16 [8, 16, 64, 8192], P('tp')
- w_up: bfloat16 [8192, 32768], P(None, 'tp')
- w_down: bfloat16 [32768, 8192], P('tp')
- k_cache: bfloat16 [256, 8, 128, 64], P('dp', 'tp'), parts along dimension 0
- v_cache: bfloat16 [256, 8, 128, 64], P('dp', 'tp'), parts along dimension 0
- positions: int32 [256], P('dp'), parts along dimension 0
Outputs:
- output 1: bfloat16 [256, 8192], P('dp'), parts along dimension 0
- output 2: bfloat16 [256, 8, 128, 64], P('dp', 'tp'), parts along dimension 0
- output 3: bfloat16 [256, 8, 128, 64], P('dp', 'tp'), parts along dimension 0
There are 4 independent parts. The reference program is written for one: setup_inputs(seed, part) draws one part's arguments, and reference() takes and returns one part's arrays. A program takes and returns all parts, laid end to end along the dimension named above; an argument that names none is the same for every part.
All inputs are finite; a program needn't handle non-finite values.
Results may differ from the reference program's by a relative error of at most 0.011894.
Values are sent between devices in bfloat16 or wider.
A program may use at most 768 MiB of HBM per device.

```python
import math
import jax
import jax.numpy as jnp
from jax import lax

D = 8192
GROUPS = 8
QPG = 16
HEAD = 64
FF = 32768
BATCH = 64
SEQ = 128

QKV_SLOTS = QPG + 2
HALF_HEAD = HEAD // 2
SCORE_SCALE = 1.0 / math.sqrt(HEAD)
LN_EPS = 1e-5
ROPE_BASE = 10000.0
NEG_BIG = -1e30


def setup_inputs(seed: int = 0, part: int = 0) -> dict:
    shared_key, part_base = jax.random.split(jax.random.key(seed))
    shared = jax.random.split(shared_key, 8)
    local = jax.random.split(jax.random.fold_in(part_base, part), 8)
    x = jax.random.normal(local[0], (BATCH, D), jnp.float32).astype(jnp.bfloat16)
    ln_attn_gamma = 1.0 + 0.3 * jax.random.normal(shared[0], (D,), jnp.float32)
    ln_attn_beta = 0.3 * jax.random.normal(shared[1], (D,), jnp.float32)
    ln_mlp_gamma = 1.0 + 0.3 * jax.random.normal(shared[2], (D,), jnp.float32)
    ln_mlp_beta = 0.3 * jax.random.normal(shared[3], (D,), jnp.float32)
    w_qkv = (jax.random.normal(shared[4], (D, GROUPS, QKV_SLOTS, HEAD), jnp.float32) * D ** -0.5).astype(jnp.bfloat16)
    w_out = (jax.random.normal(shared[5], (GROUPS, QPG, HEAD, D), jnp.float32) * (GROUPS * QPG * HEAD) ** -0.5).astype(jnp.bfloat16)
    w_up = (jax.random.normal(shared[6], (D, FF), jnp.float32) * D ** -0.5).astype(jnp.bfloat16)
    w_down = (jax.random.normal(shared[7], (FF, D), jnp.float32) * FF ** -0.5).astype(jnp.bfloat16)
    ramp = (2.0 * jnp.arange(SEQ, dtype=jnp.float32) / SEQ - 1.0)[None, None, :, None]
    k_slope = 1.5 * jax.random.normal(local[1], (BATCH, GROUPS, 1, HEAD), jnp.float32)
    k_cache = (jax.random.normal(local[2], (BATCH, GROUPS, SEQ, HEAD), jnp.float32) + ramp * k_slope).astype(jnp.bfloat16)
    v_level = jax.random.normal(local[3], (BATCH, GROUPS, 1, HEAD), jnp.float32)
    v_slope = jax.random.normal(local[4], (BATCH, GROUPS, 1, HEAD), jnp.float32)
    v_cache = (0.5 * jax.random.normal(local[5], (BATCH, GROUPS, SEQ, HEAD), jnp.float32) + v_level + ramp * v_slope).astype(jnp.bfloat16)
    positions = jax.random.randint(local[6], (BATCH,), SEQ // 4, SEQ, dtype=jnp.int32)
    positions = positions.at[0].set(SEQ - 1).at[1].set(SEQ // 4)
    return {'x': x, 'ln_attn_gamma': ln_attn_gamma, 'ln_attn_beta': ln_attn_beta, 'ln_mlp_gamma': ln_mlp_gamma, 'ln_mlp_beta': ln_mlp_beta, 'w_qkv': w_qkv, 'w_out': w_out, 'w_up': w_up, 'w_down': w_down, 'k_cache': k_cache, 'v_cache': v_cache, 'positions': positions}


def layer_norm(act_rows, ln_gamma, ln_beta):
    rows_f32 = act_rows.astype(jnp.float32)
    row_mean = jnp.mean(rows_f32, axis=-1, keepdims=True)
    centred = rows_f32 - row_mean
    row_var = jnp.mean(centred * centred, axis=-1, keepdims=True)
    return (centred * lax.rsqrt(row_var + LN_EPS) * ln_gamma + ln_beta).astype(jnp.bfloat16)


def apply_rotary(vectors, cos_t, sin_t):
    as_f32 = vectors.astype(jnp.float32)
    lower_half = as_f32[..., :HALF_HEAD]
    upper_half = as_f32[..., HALF_HEAD:]
    return jnp.concatenate([lower_half * cos_t - upper_half * sin_t, upper_half * cos_t + lower_half * sin_t], axis=-1).astype(jnp.bfloat16)


def reference(x, ln_attn_gamma, ln_attn_beta, ln_mlp_gamma, ln_mlp_beta, w_qkv, w_out, w_up, w_down, k_cache, v_cache, positions):
    attn_in = layer_norm(x, ln_attn_gamma, ln_attn_beta)
    mlp_in = layer_norm(x, ln_mlp_gamma, ln_mlp_beta)
    qkv_rows = jnp.dot(attn_in, w_qkv.reshape(D, GROUPS * QKV_SLOTS * HEAD), preferred_element_type=jnp.float32).astype(jnp.bfloat16)
    qkv_rows = qkv_rows.reshape(BATCH, GROUPS, QKV_SLOTS, HEAD)
    inv_freq = ROPE_BASE ** (-2.0 * jnp.arange(HALF_HEAD, dtype=jnp.float32) / HEAD)
    angles = positions.astype(jnp.float32)[:, None] * inv_freq[None, :]
    cos_t = jnp.cos(angles)
    sin_t = jnp.sin(angles)
    queries = apply_rotary(qkv_rows[:, :, :QPG], cos_t[:, None, None, :], sin_t[:, None, None, :])
    new_key = apply_rotary(qkv_rows[:, :, QPG], cos_t[:, None, :], sin_t[:, None, :])
    new_value = qkv_rows[:, :, QPG + 1]
    slot_ids = jnp.arange(SEQ)
    write_mask = (slot_ids[None, :] == positions[:, None])[:, None, :, None]
    keys_all = jnp.where(write_mask, new_key[:, :, None, :], k_cache)
    values_all = jnp.where(write_mask, new_value[:, :, None, :], v_cache)
    valid_mask = slot_ids[None, :] <= positions[:, None]

    def attend_group(operands):
        q_grp, k_grp, v_grp = operands
        scores = jnp.einsum('bqh,bsh->bqs', q_grp.astype(jnp.float32), k_grp.astype(jnp.float32)) * SCORE_SCALE
        scores = jnp.where(valid_mask[:, None, :], scores, NEG_BIG)
        attn_probs = jax.nn.softmax(scores, axis=-1).astype(jnp.bfloat16)
        return jnp.einsum('bqs,bsh->bqh', attn_probs.astype(jnp.float32), v_grp.astype(jnp.float32)).astype(jnp.bfloat16)

    context = lax.map(attend_group, (jnp.moveaxis(queries, 1, 0), jnp.moveaxis(keys_all, 1, 0), jnp.moveaxis(values_all, 1, 0)))
    context = jnp.moveaxis(context, 0, 1).reshape(BATCH, GROUPS * QPG * HEAD)
    attn_out = jnp.dot(context, w_out.reshape(GROUPS * QPG * HEAD, D), preferred_element_type=jnp.float32)
    hidden = jax.nn.gelu(jnp.dot(mlp_in, w_up, preferred_element_type=jnp.float32), approximate=False).astype(jnp.bfloat16)
    mlp_out = jnp.dot(hidden, w_down, preferred_element_type=jnp.float32)
    layer_out = (x.astype(jnp.float32) + attn_out + mlp_out).astype(jnp.bfloat16)
    return (layer_out, keys_all, values_all)
```

```python
import math
import numpy as np
import jax
import jax.numpy as jnp
from jax import lax
from jax.experimental import pallas as pl
from jax.experimental.pallas import tpu as pltpu
from jax.sharding import PartitionSpec as P

LN_EPS = 1e-5
ROPE_BASE = 10000.0
NEG_BIG = -1e30
F32 = jnp.float32
BF16 = jnp.bfloat16
CHUNK = 512
A_SLOTS = 4
B_SLOTS = 3


def gelu_exact(pre):
    return pre * 0.5 * (1.0 + lax.erf(pre * (1.0 / math.sqrt(2.0))))


def layer_kernel(dims, x_hbm, ga_hbm, ba_hbm, gm_hbm, bm_hbm, wqkv_hbm, wout_hbm, wup_hbm, wdown_hbm, kc_hbm, vc_hbm, pos_hbm,
                 out_hbm, ko_hbm, vo_hbm,
                 ring_a, ring_b, x_buf, attn_in, mlp_in, act, k_buf, v_buf, qkv_acc, new_kv, q_rows, ctx_rows, pre, vecs, pos_vec, pos_smem, part_buf, pair_in, sum_buf, quarter_in, out_buf,
                 sem_in, sem_qkv, sem_a, sem_b, sem_out, sem_pair, sem_quarter, sem_gather, sem_sent):
    rows, width, ff, n_query, head, seq, n_tp = dims
    qk_rows = (n_query + 2) * head
    n_qkv = width // CHUNK
    n_up = ff // CHUNK
    n_down = width // CHUNK
    ctx_w = n_query * head
    pairs = n_query // 2
    per_slot = width // qk_rows

    def qkv_row(j):
        return (j // per_slot) * width + (j % per_slot) * qk_rows

    def small_copies():
        return [
            pltpu.make_async_copy(x_hbm, x_buf, sem_in.at[0]),
            pltpu.make_async_copy(ga_hbm, vecs.at[0:1], sem_in.at[1]),
            pltpu.make_async_copy(ba_hbm, vecs.at[1:2], sem_in.at[2]),
            pltpu.make_async_copy(gm_hbm, vecs.at[2:3], sem_in.at[3]),
            pltpu.make_async_copy(bm_hbm, vecs.at[3:4], sem_in.at[4]),
            pltpu.make_async_copy(pos_hbm, pos_vec, sem_in.at[5]),
            pltpu.make_async_copy(pos_hbm, pos_smem, sem_in.at[6]),
            pltpu.make_async_copy(kc_hbm, k_buf, sem_in.at[7]),
            pltpu.make_async_copy(vc_hbm, v_buf, sem_in.at[8]),
        ]

    def qkv_copy(j):
        return pltpu.make_async_copy(wqkv_hbm.at[:, pl.ds(j * CHUNK, CHUNK)], ring_a.at[pl.ds(qkv_row(j), qk_rows), :], sem_qkv.at[j])

    def a_slot(n):
        return lax.rem(n + 3, A_SLOTS)

    def start_up(n):
        part = width // 4
        base = a_slot(n) * width
        for i in range(4):
            pltpu.make_async_copy(wup_hbm.at[pl.ds(i * part, part), pl.ds(pl.multiple_of(n * CHUNK, CHUNK), CHUNK)],
                                  ring_a.at[pl.ds(base + i * part, part), :], sem_a.at[a_slot(n)]).start()

    def wait_up(n):
        pltpu.make_async_copy(wup_hbm.at[:, pl.ds(pl.multiple_of(n * CHUNK, CHUNK), CHUNK)],
                              ring_a.at[pl.ds(a_slot(n) * width, width), :], sem_a.at[a_slot(n)]).wait()

    b_rows = ff + ctx_w

    def start_down(c):
        s = lax.rem(c, B_SLOTS)
        base = s * b_rows
        part = ff // 2
        cols = pl.ds(pl.multiple_of(c * CHUNK, CHUNK), CHUNK)
        for i in range(2):
            pltpu.make_async_copy(wdown_hbm.at[pl.ds(i * part, part), cols], ring_b.at[pl.ds(base + i * part, part), :], sem_b.at[s]).start()
        pltpu.make_async_copy(wout_hbm.at[:, cols], ring_b.at[pl.ds(base + ff, ctx_w), :], sem_b.at[s]).start()

    def wait_down(c):
        s = lax.rem(c, B_SLOTS)
        pltpu.make_async_copy(wdown_hbm.at[0:b_rows - ctx_w, pl.ds(0, CHUNK)], ring_b.at[pl.ds(s * b_rows, ff), :], sem_b.at[s]).wait()
        pltpu.make_async_copy(wout_hbm.at[:, pl.ds(0, CHUNK)], ring_b.at[pl.ds(s * b_rows + ff, ctx_w), :], sem_b.at[s]).wait()

    small = small_copies()
    for c in small:
        c.start()

    me = lax.axis_index('tp')
    n_chips = n_tp // 2
    chip, core = me // 2, lax.rem(me, 2)
    half_rows = rows // 2
    quarter = CHUNK // n_chips
    barrier = pltpu.get_barrier_semaphore()
    for d in range(1, n_tp):
        pl.semaphore_signal(barrier, inc=1, device_id={'tp': lax.rem(me + d, n_tp)}, device_id_type=pl.DeviceIdType.MESH)
    for j in range(n_qkv):
        qkv_copy(j).start()
    start_up(0)
    for c in range(B_SLOTS):
        start_down(c)

    for c in small[:5]:
        c.wait()
    lanes = 512
    n_l = width // lanes

    def fold(v):
        t = v[:, 0:128]
        for i in range(1, lanes // 128):
            t = t + v[:, i * 128:(i + 1) * 128]
        return t

    def sum_body(j, acc):
        return acc + fold(x_buf[:, pl.ds(pl.multiple_of(j * lanes, lanes), lanes)].astype(F32))

    total = lax.fori_loop(0, n_l, sum_body, jnp.zeros((rows, 128), F32))
    mean = jnp.sum(total, axis=1, keepdims=True) * (1.0 / width)

    def var_body(j, acc):
        d = x_buf[:, pl.ds(pl.multiple_of(j * lanes, lanes), lanes)].astype(F32) - mean
        return acc + fold(d * d)

    total2 = lax.fori_loop(0, n_l, var_body, jnp.zeros((rows, 128), F32))
    rstd = lax.rsqrt(jnp.sum(total2, axis=1, keepdims=True) * (1.0 / width) + LN_EPS)

    def norm_body(j, carry):
        cols = pl.ds(pl.multiple_of(j * lanes, lanes), lanes)
        nrm = (x_buf[:, cols].astype(F32) - mean) * rstd
        attn_in[0:rows, cols] = (nrm * vecs[0:1, cols] + vecs[1:2, cols]).astype(BF16)
        mlp_in[:, cols] = (nrm * vecs[2:3, cols] + vecs[3:4, cols]).astype(BF16)
        return carry

    lax.fori_loop(0, n_l, norm_body, 0)

    group = 4

    def qkv_body(g, carry):
        tot = None
        for i in range(group):
            j = g * group + i
            pltpu.make_async_copy(wqkv_hbm.at[:, pl.ds(0, CHUNK)], ring_a.at[pl.ds(0, qk_rows), :], sem_qkv.at[j]).wait()
            w = ring_a[pl.ds(pl.multiple_of(qkv_row(j), 128), qk_rows), :]
            a = attn_in[:, pl.ds(pl.multiple_of(j * CHUNK, CHUNK), CHUNK)]
            a = jnp.concatenate([a, jnp.zeros((128 - rows, CHUNK), BF16)], axis=0)
            d = lax.dot_general(w, a, (((1,), (1,)), ((), ())), preferred_element_type=F32)
            tot = d if tot is None else tot + d

        @pl.when(g == 0)
        def _():
            qkv_acc[...] = tot

        @pl.when(g > 0)
        def _():
            qkv_acc[...] += tot

        return carry

    lax.fori_loop(0, n_qkv // group, qkv_body, 0)
    for n in range(1, A_SLOTS):
        start_up(n)

    for c in small[5:]:
        c.wait()
    half = head // 2
    pos_row = jnp.concatenate([pos_vec[...], pos_vec[...]], axis=1).astype(F32)
    index = lax.broadcasted_iota(jnp.int32, (half, 128), 0).astype(F32)
    angles = jnp.exp(index * (-2.0 * math.log(ROPE_BASE) / head)) * pos_row
    cos_t = jnp.cos(angles)
    sin_t = jnp.sin(angles)

    def rotate(slot):
        u = qkv_acc[slot * head:(slot + 1) * head, :].astype(BF16).astype(F32)
        lo, hi = u[:half], u[half:]
        return jnp.concatenate([lo * cos_t - hi * sin_t, hi * cos_t + lo * sin_t], axis=0)

    for p in range(pairs):
        both = jnp.concatenate([rotate(2 * p), rotate(2 * p + 1)], axis=0)
        t = jnp.transpose(both)
        q_rows[pl.ds(p, rows, stride=pairs), :] = t[0:rows, :]
    new_kv[0:head, :] = rotate(n_query).astype(BF16)
    new_kv[head:, :] = qkv_acc[(n_query + 1) * head:, :].astype(BF16)

    scale = head ** -0.5
    lane_s = lax.broadcasted_iota(jnp.int32, (2 * head, seq), 1)
    sub_b = lax.broadcasted_iota(jnp.int32, (2 * head, seq), 0)
    lane_h = lax.broadcasted_iota(jnp.int32, (pairs, 2 * head), 1)

    def attend(b):
        pos = pos_smem[0, b]
        at_pos = lane_s == pos
        onehot = jnp.where(at_pos & (sub_b == b), 1.0, 0.0).astype(BF16)
        col = jnp.dot(new_kv[...], onehot, preferred_element_type=F32)
        r = pl.ds(pl.multiple_of(b * head, head), head)
        here = at_pos[0:head]
        keys = jnp.where(here, col[0:head], k_buf[r, :].astype(F32)).astype(BF16)
        vals = jnp.where(here, col[head:], v_buf[r, :].astype(F32)).astype(BF16)
        k_buf[r, :] = keys
        v_buf[r, :] = vals
        q2 = q_rows[pl.ds(pl.multiple_of(b * pairs, pairs), pairs), :]
        q = jnp.concatenate([jnp.where(lane_h < head, q2, 0.0), jnp.where(lane_h < head, 0.0, q2)], axis=0).astype(BF16)
        k2 = jnp.concatenate([keys, keys], axis=0)
        s = jnp.dot(q, k2, preferred_element_type=F32) * scale
        s = jnp.where(lane_s[0:2 * pairs] <= pos, s, NEG_BIG)
        e = jnp.exp(s - jnp.max(s, axis=1, keepdims=True))
        p = (e / jnp.sum(e, axis=1, keepdims=True)).astype(BF16)
        v2 = jnp.concatenate([vals, vals], axis=0)
        o = lax.dot_general(p, v2, (((1,), (1,)), ((), ())), preferred_element_type=F32)
        ctx_rows[pl.ds(pl.multiple_of(b * pairs, pairs), pairs), :] = jnp.where(lane_h < head, o[0:pairs], o[pairs:])

    batch = 8

    def attend_body(i, carry):
        for k in range(batch):
            attend(i * batch + k)
        return carry

    lax.fori_loop(0, rows // batch, attend_body, 0)
    for p in range(pairs):
        act[:, CHUNK + ff + p * 2 * head: CHUNK + ff + (p + 1) * 2 * head] = ctx_rows[pl.ds(p, rows, stride=pairs), :].astype(BF16)
    k_out = pltpu.make_async_copy(k_buf, ko_hbm, sem_out.at[0])
    v_out = pltpu.make_async_copy(v_buf, vo_hbm, sem_out.at[1])
    k_out.start()
    v_out.start()

    pre[...] = jnp.zeros_like(pre)

    def up_body(n, carry):
        @pl.when((n > 0) & (n + A_SLOTS - 1 < n_up))
        def _():
            start_up(n + A_SLOTS - 1)

        wait_up(n)
        act[:, pl.ds(pl.multiple_of(n * CHUNK, CHUNK), CHUNK)] = gelu_exact(pre[...]).astype(BF16)
        pre[...] = jnp.dot(mlp_in[...], ring_a[pl.ds(pl.multiple_of(a_slot(n) * width, width), width), :], preferred_element_type=F32)
        return carry

    lax.fori_loop(0, n_up, up_body, 0)
    act[:, ff:ff + CHUNK] = gelu_exact(pre[...]).astype(BF16)

    my_rows = pl.ds(pl.multiple_of(core * half_rows, half_rows), half_rows)
    other_rows = pl.ds(pl.multiple_of((1 - core) * half_rows, half_rows), half_rows)

    def chunk_cols(c):
        return pl.ds(pl.multiple_of(c * CHUNK, CHUNK), CHUNK)

    def quarter_cols(c, q):
        return pl.ds(pl.multiple_of(c * CHUNK + q * quarter, quarter), quarter)

    def slot_cols(c):
        return pl.ds(pl.multiple_of(c * quarter, quarter), quarter)

    def send_pair(c):
        pltpu.make_async_remote_copy(src_ref=part_buf.at[other_rows, chunk_cols(c)], dst_ref=pair_in.at[:, chunk_cols(c)],
                                     send_sem=sem_sent.at[0], recv_sem=sem_pair.at[c],
                                     device_id={'tp': chip * 2 + 1 - core}, device_id_type=pl.DeviceIdType.MESH).start()

    def send_quarters(c):
        pltpu.make_async_copy(pair_in.at[:, chunk_cols(c)], pair_in.at[:, chunk_cols(c)], sem_pair.at[c]).wait()
        both = part_buf[my_rows, chunk_cols(c)].astype(F32) + pair_in[:, chunk_cols(c)].astype(F32)
        sum_buf[:, chunk_cols(c)] = both.astype(BF16)
        for d in range(1, n_chips):
            q = lax.rem(chip + d, n_chips)
            pltpu.make_async_remote_copy(src_ref=sum_buf.at[:, quarter_cols(c, q)], dst_ref=quarter_in.at[d - 1, :, slot_cols(c)],
                                         send_sem=sem_sent.at[1], recv_sem=sem_quarter.at[d - 1, c],
                                         device_id={'tp': q * 2 + core}, device_id_type=pl.DeviceIdType.MESH).start()

    def send_result(c):
        total = x_buf[my_rows, quarter_cols(c, chip)].astype(F32) + sum_buf[:, quarter_cols(c, chip)].astype(F32)
        for d in range(1, n_chips):
            pltpu.make_async_copy(quarter_in.at[d - 1, :, slot_cols(c)], quarter_in.at[d - 1, :, slot_cols(c)], sem_quarter.at[d - 1, c]).wait()
            total = total + quarter_in[d - 1, :, slot_cols(c)].astype(F32)
        out_buf[my_rows, quarter_cols(c, chip)] = total.astype(BF16)
        for d in range(1, n_tp):
            pltpu.make_async_remote_copy(src_ref=out_buf.at[my_rows, quarter_cols(c, chip)], dst_ref=out_buf.at[my_rows, quarter_cols(c, chip)],
                                         send_sem=sem_sent.at[2], recv_sem=sem_gather.at[0],
                                         device_id={'tp': lax.rem(me + d, n_tp)}, device_id_type=pl.DeviceIdType.MESH).start()

    lag = 4
    pl.semaphore_wait(barrier, n_tp - 1)

    def down_body(c, carry):
        @pl.when((c > 0) & (c + B_SLOTS - 1 < n_down))
        def _():
            start_down(c + B_SLOTS - 1)

        wait_down(c)
        s = lax.rem(c, B_SLOTS)
        part = jnp.dot(act[:, CHUNK:], ring_b[pl.ds(pl.multiple_of(s * b_rows, 1024), b_rows), :], preferred_element_type=F32)
        part_buf[:, chunk_cols(c)] = part.astype(BF16)
        send_pair(c)

        @pl.when(c >= 1)
        def _():
            send_quarters(c - 1)

        @pl.when(c >= lag)
        def _():
            send_result(c - lag)

        return carry

    lax.fori_loop(0, n_down, down_body, 0)
    send_quarters(n_down - 1)
    for c in range(n_down - lag, n_down):
        send_result(c)

    def settle(sem, n_rows):
        pltpu.make_async_copy(out_buf.at[0:n_rows, :], out_buf.at[0:n_rows, :], sem).wait()

    settle(sem_gather.at[0], (n_tp - 1) * rows // n_tp)
    final = pltpu.make_async_copy(out_buf, out_hbm, sem_out.at[2])
    final.start()
    settle(sem_sent.at[0], rows // 2)
    settle(sem_sent.at[1], (n_chips - 1) * rows // n_tp)
    settle(sem_sent.at[2], (n_tp - 1) * rows // n_tp)
    final.wait()
    k_out.wait()
    v_out.wait()


def solution(mesh):
    row_spec = P('dp', None)
    vec_spec = P(None)
    cache_spec = P('dp', 'tp', None, None)

    def device_step(x, ga, ba, gm, bm, w_qkv, w_out, w_up, w_down, k_cache, v_cache, positions):
        rows, width = x.shape
        ff = w_up.shape[1]
        n_query, head = w_qkv.shape[2] - 2, w_qkv.shape[3]
        seq = k_cache.shape[2]
        ctx_w = n_query * head
        qk_rows = (n_query + 2) * head
        n_qkv = width // CHUNK
        n_tp = mesh.shape['tp']
        n_chips = n_tp // 2
        n_down = width // CHUNK
        dims = (rows, width, ff, n_query, head, seq, n_tp)
        wq = jnp.transpose(w_qkv, (1, 2, 3, 0)).reshape(qk_rows, width)
        wo = w_out.reshape(ctx_w, width)
        kt = jnp.transpose(k_cache, (0, 1, 3, 2)).reshape(rows * head, seq)
        vt = jnp.transpose(v_cache, (0, 1, 3, 2)).reshape(rows * head, seq)
        any_spec = pl.BlockSpec(memory_space=pl.ANY)
        out, k_new, v_new = pl.pallas_call(
            lambda *refs: layer_kernel(dims, *refs),
            name='layer',
            out_shape=(jax.ShapeDtypeStruct((rows, width), BF16), jax.ShapeDtypeStruct(kt.shape, BF16), jax.ShapeDtypeStruct(vt.shape, BF16)),
            in_specs=[any_spec] * 12,
            out_specs=(any_spec, any_spec, any_spec),
            scratch_shapes=[
                pltpu.VMEM((A_SLOTS * width, CHUNK), BF16),
                pltpu.VMEM((B_SLOTS * (ff + ctx_w), CHUNK), BF16),
                pltpu.VMEM((rows, width), BF16),
                pltpu.VMEM((rows, width), BF16),
                pltpu.VMEM((rows, width), BF16),
                pltpu.VMEM((rows, CHUNK + ff + ctx_w), BF16),
                pltpu.VMEM((rows * head, seq), BF16),
                pltpu.VMEM((rows * head, seq), BF16),
                pltpu.VMEM((qk_rows, 128), F32),
                pltpu.VMEM((2 * head, 128), BF16),
                pltpu.VMEM((rows * n_query // 2, 128), F32),
                pltpu.VMEM((rows * n_query // 2, 128), F32),
                pltpu.VMEM((rows, CHUNK), F32),
                pltpu.VMEM((4, width), F32),
                pltpu.VMEM((1, rows), jnp.int32),
                pltpu.SMEM((1, rows), jnp.int32),
                pltpu.VMEM((rows, width), BF16),
                pltpu.VMEM((rows // 2, width), BF16),
                pltpu.VMEM((rows // 2, width), BF16),
                pltpu.VMEM((n_chips - 1, rows // 2, width // n_chips), BF16),
                pltpu.VMEM((rows, width), BF16),
                pltpu.SemaphoreType.DMA((9,)),
                pltpu.SemaphoreType.DMA((n_qkv,)),
                pltpu.SemaphoreType.DMA((A_SLOTS,)),
                pltpu.SemaphoreType.DMA((B_SLOTS,)),
                pltpu.SemaphoreType.DMA((3,)),
                pltpu.SemaphoreType.DMA((n_down,)),
                pltpu.SemaphoreType.DMA((n_chips - 1, n_down)),
                pltpu.SemaphoreType.DMA((1,)),
                pltpu.SemaphoreType.DMA((3,)),
            ],
            compiler_params=pltpu.CompilerParams(vmem_limit_bytes=67043328, collective_id=0, has_side_effects=True),
        )(x, ga.reshape(1, width), ba.reshape(1, width), gm.reshape(1, width), bm.reshape(1, width), wq, wo, w_up, w_down, kt, vt, positions.reshape(1, rows))
        k_new = jnp.transpose(k_new.reshape(rows, 1, head, seq), (0, 1, 3, 2))
        v_new = jnp.transpose(v_new.reshape(rows, 1, head, seq), (0, 1, 3, 2))
        return out, k_new, v_new

    return jax.shard_map(device_step, mesh=mesh, in_specs=(row_spec, vec_spec, vec_spec, vec_spec, vec_spec, P(None, 'tp', None, None), P('tp', None, None, None), P(None, 'tp'), P('tp', None), cache_spec, cache_spec, P('dp')), out_specs=(row_spec, cache_spec, cache_spec), check_vma=False)
```

```python
import math
import numpy as np
import jax
import jax.numpy as jnp
from jax import lax
from jax.experimental import pallas as pl
from jax.experimental.pallas import tpu as pltpu
from jax.sharding import PartitionSpec as P

LN_EPS = 1e-5
ROPE_BASE = 10000.0
NEG_BIG = -1e30
F32 = jnp.float32
BF16 = jnp.bfloat16
CHUNK = 512
A_SLOTS = 4
B_SLOTS = 3
N_DIRECT = 2


def gelu_exact(pre):
    return pre * 0.5 * (1.0 + lax.erf(pre * (1.0 / math.sqrt(2.0))))


def layer_kernel(dims, x_hbm, ga_hbm, ba_hbm, gm_hbm, bm_hbm, wqkv_hbm, wout_hbm, wup_hbm, wdown_hbm, kc_hbm, vc_hbm, pos_hbm,
                 out_buf, k_buf, v_buf,
                 ring, x_buf, attn_in, mlp_in, act, qkv_acc, new_kv, q_rows, ctx_rows, pre, vecs, pos_vec, pos_smem, part_buf, pair_in, sum_buf, quarter_in, last_in,
                 sem_in, sem_qkv, sem_a, sem_b, sem_pair, sem_quarter, sem_gather, sem_last, sem_sent):
    rows, width, ff, n_query, head, seq, n_tp = dims
    qk_rows = (n_query + 2) * head
    n_qkv = width // CHUNK
    n_up = ff // CHUNK
    n_down = width // CHUNK
    ctx_w = n_query * head
    pairs = n_query // 2
    per_slot = width // qk_rows

    def qkv_row(j):
        return (j // per_slot) * width + (j % per_slot) * qk_rows

    def small_copies():
        return [
            pltpu.make_async_copy(x_hbm, x_buf, sem_in.at[0]),
            pltpu.make_async_copy(ga_hbm, vecs.at[0:1], sem_in.at[1]),
            pltpu.make_async_copy(ba_hbm, vecs.at[1:2], sem_in.at[2]),
            pltpu.make_async_copy(gm_hbm, vecs.at[2:3], sem_in.at[3]),
            pltpu.make_async_copy(bm_hbm, vecs.at[3:4], sem_in.at[4]),
            pltpu.make_async_copy(pos_hbm, pos_vec, sem_in.at[5]),
            pltpu.make_async_copy(pos_hbm, pos_smem, sem_in.at[6]),
            pltpu.make_async_copy(kc_hbm, k_buf, sem_in.at[7]),
            pltpu.make_async_copy(vc_hbm, v_buf, sem_in.at[8]),
        ]

    def qkv_copy(j):
        return pltpu.make_async_copy(wqkv_hbm.at[:, pl.ds(j * CHUNK, CHUNK)], ring.at[pl.ds(qkv_row(j), qk_rows), :], sem_qkv.at[j])

    def a_slot(n):
        return lax.rem(n + 3, A_SLOTS)

    def start_up(n):
        part = width // 4
        base = a_slot(n) * width
        for i in range(4):
            pltpu.make_async_copy(wup_hbm.at[pl.ds(i * part, part), pl.ds(pl.multiple_of(n * CHUNK, CHUNK), CHUNK)],
                                  ring.at[pl.ds(base + i * part, part), :], sem_a.at[a_slot(n)]).start()

    def wait_up(n):
        pltpu.make_async_copy(wup_hbm.at[:, pl.ds(pl.multiple_of(n * CHUNK, CHUNK), CHUNK)],
                              ring.at[pl.ds(a_slot(n) * width, width), :], sem_a.at[a_slot(n)]).wait()

    b_rows = ff + ctx_w
    n_slots = A_SLOTS + B_SLOTS
    parts = ((0, ff // 2), (ff // 2, ff // 2), (ff, ctx_w))

    def down_base(c):
        s = lax.rem(c, n_slots)
        large = lax.rem(a_slot(n_up - A_SLOTS) + s - B_SLOTS + A_SLOTS, A_SLOTS) * width
        return pl.multiple_of(jnp.where(s < B_SLOTS, A_SLOTS * width + s * b_rows, large), 1024)

    def down_copy(c, i):
        first, count = parts[i]
        cols = pl.ds(pl.multiple_of(c * CHUNK, CHUNK), CHUNK)
        src = wout_hbm.at[:, cols] if i == 2 else wdown_hbm.at[pl.ds(first, count), cols]
        return pltpu.make_async_copy(src, ring.at[pl.ds(down_base(c) + first, count), :], sem_b.at[lax.rem(c, n_slots), i])

    def start_down(c):
        for i in range(len(parts)):
            down_copy(c, i).start()

    small = small_copies()
    for c in small[:7]:
        c.start()

    me = lax.axis_index('tp')
    n_chips = n_tp // 2
    chip, core = me // 2, lax.rem(me, 2)
    half_rows = rows // 2
    quarter = CHUNK // n_chips
    barrier = pltpu.get_barrier_semaphore()
    for d in range(1, n_tp):
        pl.semaphore_signal(barrier, inc=1, device_id={'tp': lax.rem(me + d, n_tp)}, device_id_type=pl.DeviceIdType.MESH)
    for j in range(n_qkv):
        qkv_copy(j).start()

    for c in small[:5]:
        c.wait()
    lanes = 512
    n_l = width // lanes

    def fold(v):
        t = v[:, 0:128]
        for i in range(1, lanes // 128):
            t = t + v[:, i * 128:(i + 1) * 128]
        return t

    def sum_body(j, acc):
        return acc + fold(x_buf[:, pl.ds(pl.multiple_of(j * lanes, lanes), lanes)].astype(F32))

    total = lax.fori_loop(0, n_l, sum_body, jnp.zeros((rows, 128), F32))
    mean = jnp.sum(total, axis=1, keepdims=True) * (1.0 / width)

    def var_body(j, acc):
        d = x_buf[:, pl.ds(pl.multiple_of(j * lanes, lanes), lanes)].astype(F32) - mean
        return acc + fold(d * d)

    total2 = lax.fori_loop(0, n_l, var_body, jnp.zeros((rows, 128), F32))
    rstd = lax.rsqrt(jnp.sum(total2, axis=1, keepdims=True) * (1.0 / width) + LN_EPS)

    def norm_body(j, carry):
        cols = pl.ds(pl.multiple_of(j * lanes, lanes), lanes)
        nrm = (x_buf[:, cols].astype(F32) - mean) * rstd
        attn_in[0:rows, cols] = (nrm * vecs[0:1, cols] + vecs[1:2, cols]).astype(BF16)
        mlp_in[:, cols] = (nrm * vecs[2:3, cols] + vecs[3:4, cols]).astype(BF16)
        return carry

    with jax.named_scope('norm'):
        lax.fori_loop(0, n_l, norm_body, 0)

    group = 4

    def qkv_step(g):
        tot = None
        for i in range(group):
            j = g * group + i
            with jax.named_scope('qkv_wait'):
                pltpu.make_async_copy(wqkv_hbm.at[:, pl.ds(0, CHUNK)], ring.at[pl.ds(0, qk_rows), :], sem_qkv.at[j]).wait()
            w = ring[qkv_row(j):qkv_row(j) + qk_rows, :]
            a = attn_in[:, j * CHUNK:(j + 1) * CHUNK]
            d = lax.dot_general(a, w, (((1,), (1,)), ((), ())), preferred_element_type=F32)
            tot = d if tot is None else tot + d

        qkv_acc[...] = tot if g == 0 else qkv_acc[...] + tot

    for g in range(n_qkv // group):
        if g == 0:
            small[7].start()
            small[8].start()
            start_up(0)
        if g == 2:
            start_up(1)
        with jax.named_scope('qkv'):
            qkv_step(g)
    for n in range(2, A_SLOTS):
        start_up(n)
    start_down(0)

    for c in small[5:]:
        c.wait()
    half = head // 2
    pair_w = 2 * head
    pos_row = jnp.concatenate([pos_vec[...], pos_vec[...]], axis=1).astype(F32)
    pos_col = jnp.transpose(jnp.broadcast_to(pos_row, (128, 128)))[0:rows, :]
    lane = lax.broadcasted_iota(jnp.int32, (rows, pair_w), 1)
    first_half = lax.rem(lane, head) < half
    angles = jnp.exp(lax.rem(lane, half).astype(F32) * (-2.0 * math.log(ROPE_BASE) / head)) * pos_col
    cos_t = jnp.cos(angles)
    sin_t = jnp.where(first_half, -jnp.sin(angles), jnp.sin(angles))

    def rotate(u):
        swapped = jnp.where(first_half, pltpu.roll(u, pair_w - half, axis=1), pltpu.roll(u, half, axis=1))
        return u * cos_t + swapped * sin_t

    for p in range(pairs):
        q_rows[pl.ds(p, rows, stride=pairs), :] = rotate(qkv_acc[:, p * pair_w:(p + 1) * pair_w].astype(BF16).astype(F32))
    kv = qkv_acc[:, pairs * pair_w:].astype(BF16).astype(F32)
    kv = jnp.where(lane < head, rotate(kv), kv)
    new_kv[...] = jnp.transpose(jnp.concatenate([kv, jnp.zeros((128 - rows, pair_w), F32)], axis=0)).astype(BF16)

    scale = head ** -0.5
    lane_s = lax.broadcasted_iota(jnp.int32, (2 * head, seq), 1)
    sub_b = lax.broadcasted_iota(jnp.int32, (2 * head, seq), 0)
    lane_h = lax.broadcasted_iota(jnp.int32, (pairs, 2 * head), 1)

    batch = 8

    def attend_body(i, carry):
        bs = [i * batch + k for k in range(batch)]
        at = [pl.ds(pl.multiple_of(b * head, head), head) for b in bs]
        rr = [pl.ds(pl.multiple_of(b * pairs, pairs), pairs) for b in bs]
        k_old = [k_buf[r, :] for r in at]
        v_old = [v_buf[r, :] for r in at]
        q2 = [q_rows[r, :] for r in rr]
        pos = [pos_smem[0, b] for b in bs]
        pick = jnp.concatenate([jnp.where(sub_b == b, 1.0, 0.0).astype(BF16) for b in bs], axis=1)
        col = jnp.dot(new_kv[...], pick, preferred_element_type=F32)
        keys, vals, scores = [], [], []
        for k in range(batch):
            here = lane_s[0:head] == pos[k]
            c = col[:, k * seq:(k + 1) * seq]
            keys.append(jnp.where(here, c[0:head], k_old[k].astype(F32)).astype(BF16))
            vals.append(jnp.where(here, c[head:], v_old[k].astype(F32)).astype(BF16))
        for k in range(batch):
            q = jnp.concatenate([jnp.where(lane_h < head, q2[k], 0.0), jnp.where(lane_h < head, 0.0, q2[k])], axis=0).astype(BF16)
            s = jnp.dot(q, jnp.concatenate([keys[k], keys[k]], axis=0), preferred_element_type=F32) * scale
            scores.append(jnp.where(lane_s[0:2 * pairs] <= pos[k], s, NEG_BIG))
        top = [jnp.max(s, axis=1, keepdims=True) for s in scores]
        e = [jnp.exp(s - m) for s, m in zip(scores, top)]
        den = [jnp.sum(x, axis=1, keepdims=True) for x in e]
        p = [(x / d).astype(BF16) for x, d in zip(e, den)]
        o = [lax.dot_general(p[k], jnp.concatenate([vals[k], vals[k]], axis=0), (((1,), (1,)), ((), ())), preferred_element_type=F32) for k in range(batch)]
        for k in range(batch):
            ctx_rows[rr[k], :] = jnp.where(lane_h < head, o[k][0:pairs], o[k][pairs:])
        for k in range(batch):
            k_buf[at[k], :] = keys[k]
            v_buf[at[k], :] = vals[k]
        return carry

    with jax.named_scope('attend'):
        lax.fori_loop(0, rows // batch, attend_body, 0)
    for p in range(pairs):
        act[:, CHUNK + ff + p * 2 * head: CHUNK + ff + (p + 1) * 2 * head] = ctx_rows[pl.ds(p, rows, stride=pairs), :].astype(BF16)

    pre[...] = jnp.zeros_like(pre)

    def up_body(n, carry):
        @pl.when((n > 0) & (n + A_SLOTS - 1 < n_up))
        def _():
            start_up(n + A_SLOTS - 1)

        @pl.when(n + A_SLOTS - 1 == n_up)
        def _():
            for c in range(1, B_SLOTS):
                start_down(c)

        @pl.when(n + A_SLOTS - 1 >= n_up)
        def _():
            start_down(n + A_SLOTS - 1 - n_up + B_SLOTS)

        with jax.named_scope('up_wait'):
            wait_up(n)
        act[:, pl.ds(pl.multiple_of(n * CHUNK, CHUNK), CHUNK)] = gelu_exact(pre[...]).astype(BF16)
        pre[...] = jnp.dot(mlp_in[...], ring[pl.ds(pl.multiple_of(a_slot(n) * width, width), width), :], preferred_element_type=F32)
        return carry

    with jax.named_scope('up'):
        lax.fori_loop(0, n_up, up_body, 0)
    act[:, ff:ff + CHUNK] = gelu_exact(pre[...]).astype(BF16)

    n_paired = n_down - N_DIRECT
    my_rows = pl.ds(pl.multiple_of(core * half_rows, half_rows), half_rows)
    other_rows = pl.ds(pl.multiple_of((1 - core) * half_rows, half_rows), half_rows)

    def chunk_cols(c):
        return pl.ds(pl.multiple_of(c * CHUNK, CHUNK), CHUNK)

    def quarter_cols(c, q):
        return pl.ds(pl.multiple_of(c * CHUNK + q * quarter, quarter), quarter)

    def slot_cols(c):
        return pl.ds(pl.multiple_of(c * quarter, quarter), quarter)

    def send_pair(c):
        pltpu.make_async_remote_copy(src_ref=part_buf.at[other_rows, chunk_cols(c)], dst_ref=pair_in.at[:, chunk_cols(c)],
                                     send_sem=sem_sent.at[0], recv_sem=sem_pair.at[c],
                                     device_id={'tp': chip * 2 + 1 - core}, device_id_type=pl.DeviceIdType.MESH).start()

    def send_quarters(c):
        pltpu.make_async_copy(pair_in.at[:, chunk_cols(c)], pair_in.at[:, chunk_cols(c)], sem_pair.at[c]).wait()
        both = part_buf[my_rows, chunk_cols(c)].astype(F32) + pair_in[:, chunk_cols(c)].astype(F32)
        sum_buf[:, chunk_cols(c)] = both.astype(BF16)
        for d in sorted(range(1, n_chips), key=lambda d: -min(d, n_chips - d)):
            q = lax.rem(chip + d, n_chips)
            pltpu.make_async_remote_copy(src_ref=sum_buf.at[:, quarter_cols(c, q)], dst_ref=quarter_in.at[d - 1, :, slot_cols(c)],
                                         send_sem=sem_sent.at[1], recv_sem=sem_quarter.at[d - 1, c],
                                         device_id={'tp': q * 2 + core}, device_id_type=pl.DeviceIdType.MESH).start()

    def send_result(c):
        total = x_buf[my_rows, quarter_cols(c, chip)].astype(F32) + sum_buf[:, quarter_cols(c, chip)].astype(F32)
        for d in range(1, n_chips):
            pltpu.make_async_copy(quarter_in.at[d - 1, :, slot_cols(c)], quarter_in.at[d - 1, :, slot_cols(c)], sem_quarter.at[d - 1, c]).wait()
            total = total + quarter_in[d - 1, :, slot_cols(c)].astype(F32)
        gather(c, total)

    def gather(c, total):
        out_buf[my_rows, quarter_cols(c, chip)] = total.astype(BF16)
        for d in sorted(range(1, n_tp), key=lambda d: -min(d, n_tp - d)):
            pltpu.make_async_remote_copy(src_ref=out_buf.at[my_rows, quarter_cols(c, chip)], dst_ref=out_buf.at[my_rows, quarter_cols(c, chip)],
                                         send_sem=sem_sent.at[2], recv_sem=sem_gather.at[0],
                                         device_id={'tp': lax.rem(me + d, n_tp)}, device_id_type=pl.DeviceIdType.MESH).start()

    def send_direct(c):
        for d in sorted(range(1, n_tp), key=lambda d: -min(d, n_tp - d)):
            to = lax.rem(me + d, n_tp)
            src = part_buf.at[pl.ds(pl.multiple_of(lax.rem(to, 2) * half_rows, half_rows), half_rows), quarter_cols(c, to // 2)]
            pltpu.make_async_remote_copy(src_ref=src, dst_ref=last_in.at[c - n_paired, d - 1], send_sem=sem_sent.at[3], recv_sem=sem_last.at[c - n_paired, d - 1],
                                         device_id={'tp': to}, device_id_type=pl.DeviceIdType.MESH).start()

    def send_result_direct(c):
        total = x_buf[my_rows, quarter_cols(c, chip)].astype(F32) + part_buf[my_rows, quarter_cols(c, chip)].astype(F32)
        for d in range(1, n_tp):
            pltpu.make_async_copy(last_in.at[c - n_paired, d - 1], last_in.at[c - n_paired, d - 1], sem_last.at[c - n_paired, d - 1]).wait()
            total = total + last_in[c - n_paired, d - 1].astype(F32)
        gather(c, total)

    lag = 4
    pl.semaphore_wait(barrier, n_tp - 1)
    start_down(n_slots - 1)

    def multiply(c, groups):
        total = None
        for group in groups:
            with jax.named_scope('down_wait'):
                for i in group:
                    down_copy(c, i).wait()
            first, count = parts[group[0]][0], sum(parts[i][1] for i in group)
            w = ring[pl.ds(down_base(c) + first, count), :]
            d = jnp.dot(act[:, CHUNK + first:CHUNK + first + count], w, preferred_element_type=F32)
            total = d if total is None else total + d
        part_buf[:, chunk_cols(c)] = total.astype(BF16)

    def down_body(c, carry):
        @pl.when((c > 0) & (c + n_slots - 1 < n_down))
        def _():
            start_down(c + n_slots - 1)

        multiply(c, ((0, 1, 2),))
        send_pair(c)

        @pl.when(c >= 1)
        def _():
            with jax.named_scope('quarters'):
                send_quarters(c - 1)

        @pl.when(c >= lag)
        def _():
            with jax.named_scope('result'):
                send_result(c - lag)

        return carry

    with jax.named_scope('down'):
        lax.fori_loop(0, n_paired, down_body, 0)
    done = n_paired - lag
    for c in range(n_paired, n_down):
        with jax.named_scope('tail_multiply'):
            multiply(c, ((0, 1, 2),) if c < n_down - 1 else ((0,), (1,), (2,)))
        send_direct(c)
        if c == n_paired:
            with jax.named_scope('tail_quarters'):
                send_quarters(c - 1)
        with jax.named_scope('tail_result'):
            send_result(done)
        done += 1
    for c in range(done, n_paired):
        with jax.named_scope('tail_result'):
            send_result(c)
    for c in range(n_paired, n_down):
        with jax.named_scope('tail_direct'):
            send_result_direct(c)

    def settle(sem, n_rows):
        pltpu.make_async_copy(out_buf.at[0:n_rows, :], out_buf.at[0:n_rows, :], sem).wait()

    with jax.named_scope('gather_wait'):
        settle(sem_gather.at[0], (n_tp - 1) * rows // n_tp)
    with jax.named_scope('sent_wait'):
        sent = pltpu.make_async_copy(part_buf.at[other_rows, 0:n_paired * CHUNK], part_buf.at[other_rows, 0:n_paired * CHUNK], sem_sent.at[0])
        sent.wait()
        for d in range(1, n_chips):
            pltpu.make_async_copy(quarter_in.at[d - 1, :, 0:n_paired * quarter], quarter_in.at[d - 1, :, 0:n_paired * quarter], sem_sent.at[1]).wait()
        settle(sem_sent.at[2], (n_tp - 1) * rows // n_tp)
        pltpu.make_async_copy(last_in, last_in, sem_sent.at[3]).wait()


def write_kernel(a_ref, b_ref, c_ref, a_out, b_out, c_out, sem):
    copies = []
    for i, (src, dst) in enumerate(((a_ref, a_out), (b_ref, b_out), (c_ref, c_out))):
        copies.append(pltpu.make_async_copy(src, dst, sem.at[i]))
    for c in copies:
        c.start()
    for c in copies:
        c.wait()


def solution(mesh):
    row_spec = P('dp', None)
    vec_spec = P(None)
    cache_spec = P('dp', 'tp', None, None)

    def device_step(x, ga, ba, gm, bm, w_qkv, w_out, w_up, w_down, k_cache, v_cache, positions):
        rows, width = x.shape
        ff = w_up.shape[1]
        n_query, head = w_qkv.shape[2] - 2, w_qkv.shape[3]
        seq = k_cache.shape[2]
        ctx_w = n_query * head
        qk_rows = (n_query + 2) * head
        n_qkv = width // CHUNK
        n_tp = mesh.shape['tp']
        n_chips = n_tp // 2
        n_down = width // CHUNK
        dims = (rows, width, ff, n_query, head, seq, n_tp)
        wq = jnp.transpose(w_qkv, (1, 2, 3, 0)).reshape(qk_rows, width)
        wo = w_out.reshape(ctx_w, width)
        kt = jnp.transpose(k_cache, (0, 1, 3, 2)).reshape(rows * head, seq)
        vt = jnp.transpose(v_cache, (0, 1, 3, 2)).reshape(rows * head, seq)
        any_spec = pl.BlockSpec(memory_space=pl.ANY)
        vmem_spec = pl.BlockSpec(memory_space=pltpu.VMEM)
        out, k_new, v_new = pl.pallas_call(
            lambda *refs: layer_kernel(dims, *refs),
            name='layer',
            out_shape=(pltpu.VMEM((rows, width), BF16), pltpu.VMEM(kt.shape, BF16), pltpu.VMEM(vt.shape, BF16)),
            in_specs=[any_spec] * 12,
            out_specs=(vmem_spec, vmem_spec, vmem_spec),
            scratch_shapes=[
                pltpu.VMEM((A_SLOTS * width + B_SLOTS * (ff + ctx_w), CHUNK), BF16),
                pltpu.VMEM((rows, width), BF16),
                pltpu.VMEM((rows, width), BF16),
                pltpu.VMEM((rows, width), BF16),
                pltpu.VMEM((rows, CHUNK + ff + ctx_w), BF16),
                pltpu.VMEM((rows, qk_rows), F32),
                pltpu.VMEM((2 * head, 128), BF16),
                pltpu.VMEM((rows * n_query // 2, 128), F32),
                pltpu.VMEM((rows * n_query // 2, 128), F32),
                pltpu.VMEM((rows, CHUNK), F32),
                pltpu.VMEM((4, width), F32),
                pltpu.VMEM((1, rows), jnp.int32),
                pltpu.SMEM((1, rows), jnp.int32),
                pltpu.VMEM((rows, width), BF16),
                pltpu.VMEM((rows // 2, width), BF16),
                pltpu.VMEM((rows // 2, width), BF16),
                pltpu.VMEM((n_chips - 1, rows // 2, width // n_chips), BF16),
                pltpu.VMEM((N_DIRECT, n_tp - 1, rows // 2, CHUNK // n_chips), BF16),
                pltpu.SemaphoreType.DMA((9,)),
                pltpu.SemaphoreType.DMA((n_qkv,)),
                pltpu.SemaphoreType.DMA((A_SLOTS,)),
                pltpu.SemaphoreType.DMA((A_SLOTS + B_SLOTS, 3)),
                pltpu.SemaphoreType.DMA((n_down,)),
                pltpu.SemaphoreType.DMA((n_chips - 1, n_down)),
                pltpu.SemaphoreType.DMA((1,)),
                pltpu.SemaphoreType.DMA((N_DIRECT, n_tp - 1)),
                pltpu.SemaphoreType.DMA((4,)),
            ],
            compiler_params=pltpu.CompilerParams(vmem_limit_bytes=60 * 1024 * 1024, collective_id=0, has_side_effects=True),
        )(x, ga.reshape(1, width), ba.reshape(1, width), gm.reshape(1, width), bm.reshape(1, width), wq, wo, w_up, w_down, kt, vt, positions.reshape(1, rows))
        out, k_new, v_new = (pltpu.with_memory_space_constraint(v, pltpu.VMEM) for v in (out, k_new, v_new))
        out, k_new, v_new = pl.pallas_call(
            write_kernel,
            name='write',
            out_shape=(jax.ShapeDtypeStruct((rows, width), BF16), jax.ShapeDtypeStruct(kt.shape, BF16), jax.ShapeDtypeStruct(vt.shape, BF16)),
            in_specs=[vmem_spec] * 3,
            out_specs=(any_spec, any_spec, any_spec),
            scratch_shapes=[pltpu.SemaphoreType.DMA((3,))],
            compiler_params=pltpu.CompilerParams(vmem_limit_bytes=1024 * 1024),
        )(out, k_new, v_new)
        k_new = jnp.transpose(k_new.reshape(rows, 1, head, seq), (0, 1, 3, 2))
        v_new = jnp.transpose(v_new.reshape(rows, 1, head, seq), (0, 1, 3, 2))
        return out, k_new, v_new

    return jax.shard_map(device_step, mesh=mesh, in_specs=(row_spec, vec_spec, vec_spec, vec_spec, vec_spec, P(None, 'tp', None, None), P('tp', None, None, None), P(None, 'tp'), P('tp', None), cache_spec, cache_spec, P('dp')), out_specs=(row_spec, cache_spec, cache_spec), check_vma=False)
```

```python
import math
import numpy as np
import jax
import jax.numpy as jnp
from jax import lax
from jax.experimental import pallas as pl
from jax.experimental.pallas import tpu as pltpu
from jax.sharding import PartitionSpec as P

LN_EPS = 1e-5
ROPE_BASE = 10000.0
NEG_BIG = -1e30
F32 = jnp.float32
BF16 = jnp.bfloat16
CHUNK = 512
A_SLOTS = 4
B_SLOTS = 3
N_DIRECT = 2
QKV_GROUP = 4


def gelu_exact(pre):
    return pre * 0.5 * (1.0 + lax.erf(pre * (1.0 / math.sqrt(2.0))))


def layer_kernel(dims, x_hbm, ga_hbm, ba_hbm, gm_hbm, bm_hbm, wqkv_hbm, wout_hbm, wup_hbm, wdown_hbm, kc_hbm, vc_hbm, pos_hbm,
                 out_buf, k_buf, v_buf,
                 ring, x_buf, attn_in, mlp_in, act, qkv_acc, new_kv, q_rows, ctx_rows, pre, vecs, pos_vec, pos_smem, part_buf, pair_in, sum_buf, quarter_in, last_in,
                 sem_in, sem_qkv, sem_a, sem_b, sem_pair, sem_quarter, sem_gather, sem_last, sem_sent):
    rows, width, ff, n_query, head, seq, n_tp = dims
    qk_rows = (n_query + 2) * head
    n_qkv = width // CHUNK
    n_up = ff // CHUNK
    n_down = width // CHUNK
    ctx_w = n_query * head
    pairs = n_query // 2
    per_slot = width // qk_rows
    group = QKV_GROUP

    def qkv_row(j):
        return (j // per_slot) * width + (j % per_slot) * qk_rows

    def small_copies():
        return [
            pltpu.make_async_copy(x_hbm, x_buf, sem_in.at[0]),
            pltpu.make_async_copy(ga_hbm, vecs.at[0:1], sem_in.at[1]),
            pltpu.make_async_copy(ba_hbm, vecs.at[1:2], sem_in.at[1]),
            pltpu.make_async_copy(gm_hbm, vecs.at[2:3], sem_in.at[1]),
            pltpu.make_async_copy(bm_hbm, vecs.at[3:4], sem_in.at[1]),
            pltpu.make_async_copy(pos_hbm, pos_vec, sem_in.at[2]),
            pltpu.make_async_copy(pos_hbm, pos_smem, sem_in.at[3]),
            pltpu.make_async_copy(kc_hbm, k_buf, sem_in.at[4]),
            pltpu.make_async_copy(vc_hbm, v_buf, sem_in.at[4]),
        ]

    def qkv_copy(j):
        return pltpu.make_async_copy(wqkv_hbm.at[:, pl.ds(j * CHUNK, CHUNK)], ring.at[pl.ds(qkv_row(j), qk_rows), :], sem_qkv.at[j // group])

    def a_slot(n):
        return lax.rem(n + 3, A_SLOTS)

    def start_up(n):
        part = width // 4
        base = a_slot(n) * width
        for i in range(4):
            pltpu.make_async_copy(wup_hbm.at[pl.ds(i * part, part), pl.ds(pl.multiple_of(n * CHUNK, CHUNK), CHUNK)],
                                  ring.at[pl.ds(base + i * part, part), :], sem_a.at[a_slot(n)]).start()

    def wait_up(n):
        pltpu.make_async_copy(wup_hbm.at[:, pl.ds(pl.multiple_of(n * CHUNK, CHUNK), CHUNK)],
                              ring.at[pl.ds(a_slot(n) * width, width), :], sem_a.at[a_slot(n)]).wait()

    b_rows = ff + ctx_w
    n_slots = A_SLOTS + B_SLOTS
    parts = ((0, ff // 2), (ff // 2, ff // 2), (ff, ctx_w))

    def down_base(c):
        s = lax.rem(c, n_slots)
        large = lax.rem(a_slot(n_up - A_SLOTS) + s - B_SLOTS + A_SLOTS, A_SLOTS) * width
        return pl.multiple_of(jnp.where(s < B_SLOTS, A_SLOTS * width + s * b_rows, large), 1024)

    def down_copy(c, i, sem):
        first, count = parts[i]
        cols = pl.ds(pl.multiple_of(c * CHUNK, CHUNK), CHUNK)
        src = wout_hbm.at[:, cols] if i == 2 else wdown_hbm.at[pl.ds(first, count), cols]
        return pltpu.make_async_copy(src, ring.at[pl.ds(down_base(c) + first, count), :], sem)

    def start_down(c):
        for i in range(len(parts)):
            down_copy(c, i, sem_b.at[lax.rem(c, n_slots)]).start()

    def start_last_down():
        for i in range(len(parts)):
            down_copy(n_down - 1, i, sem_b.at[n_slots + i]).start()

    small = small_copies()
    for c in small[:7]:
        c.start()

    me = lax.axis_index('tp')
    n_chips = n_tp // 2
    chip, core = me // 2, lax.rem(me, 2)
    half_rows = rows // 2
    quarter = CHUNK // n_chips
    barrier = pltpu.get_barrier_semaphore()
    for d in range(1, n_tp):
        pl.semaphore_signal(barrier, inc=1, device_id={'tp': lax.rem(me + d, n_tp)}, device_id_type=pl.DeviceIdType.MESH)
    for j in range(n_qkv):
        qkv_copy(j).start()

    for c in small[:5]:
        c.wait()
    lanes = 512
    n_l = width // lanes

    def fold(v):
        t = v[:, 0:128]
        for i in range(1, lanes // 128):
            t = t + v[:, i * 128:(i + 1) * 128]
        return t

    def sum_body(j, acc):
        return acc + fold(x_buf[:, pl.ds(pl.multiple_of(j * lanes, lanes), lanes)].astype(F32))

    total = lax.fori_loop(0, n_l, sum_body, jnp.zeros((rows, 128), F32))
    mean = jnp.sum(total, axis=1, keepdims=True) * (1.0 / width)

    def var_body(j, acc):
        d = x_buf[:, pl.ds(pl.multiple_of(j * lanes, lanes), lanes)].astype(F32) - mean
        return acc + fold(d * d)

    total2 = lax.fori_loop(0, n_l, var_body, jnp.zeros((rows, 128), F32))
    rstd = lax.rsqrt(jnp.sum(total2, axis=1, keepdims=True) * (1.0 / width) + LN_EPS)

    def norm_body(j, carry):
        cols = pl.ds(pl.multiple_of(j * lanes, lanes), lanes)
        nrm = (x_buf[:, cols].astype(F32) - mean) * rstd
        attn_in[0:rows, cols] = (nrm * vecs[0:1, cols] + vecs[1:2, cols]).astype(BF16)
        mlp_in[:, cols] = (nrm * vecs[2:3, cols] + vecs[3:4, cols]).astype(BF16)
        return carry

    with jax.named_scope('norm'):
        lax.fori_loop(0, n_l, norm_body, 0)


    def qkv_step(g):
        tot = None
        with jax.named_scope('qkv_wait'):
            for i in range(group):
                qkv_copy(g * group + i).wait()
        for i in range(group):
            j = g * group + i
            w = ring[qkv_row(j):qkv_row(j) + qk_rows, :]
            a = attn_in[:, j * CHUNK:(j + 1) * CHUNK]
            d = lax.dot_general(a, w, (((1,), (1,)), ((), ())), preferred_element_type=F32)
            tot = d if tot is None else tot + d

        qkv_acc[...] = tot if g == 0 else qkv_acc[...] + tot

    for g in range(n_qkv // group):
        if g == 0:
            small[7].start()
            small[8].start()
            start_up(0)
        if g == 2:
            start_up(1)
        with jax.named_scope('qkv'):
            qkv_step(g)
    for n in range(2, A_SLOTS):
        start_up(n)
    start_down(0)

    for c in small[5:]:
        c.wait()
    half = head // 2
    pair_w = 2 * head
    pos_row = jnp.concatenate([pos_vec[...], pos_vec[...]], axis=1).astype(F32)
    pos_col = jnp.transpose(jnp.broadcast_to(pos_row, (128, 128)))[0:rows, :]
    lane = lax.broadcasted_iota(jnp.int32, (rows, pair_w), 1)
    first_half = lax.rem(lane, head) < half
    angles = jnp.exp(lax.rem(lane, half).astype(F32) * (-2.0 * math.log(ROPE_BASE) / head)) * pos_col
    cos_t = jnp.cos(angles)
    sin_t = jnp.where(first_half, -jnp.sin(angles), jnp.sin(angles))

    def rotate(u):
        swapped = jnp.where(first_half, pltpu.roll(u, pair_w - half, axis=1), pltpu.roll(u, half, axis=1))
        return u * cos_t + swapped * sin_t

    for p in range(pairs):
        q_rows[pl.ds(p, rows, stride=pairs), :] = rotate(qkv_acc[:, p * pair_w:(p + 1) * pair_w].astype(BF16).astype(F32))
    kv = qkv_acc[:, pairs * pair_w:].astype(BF16).astype(F32)
    kv = jnp.where(lane < head, rotate(kv), kv)
    new_kv[...] = jnp.transpose(jnp.concatenate([kv, jnp.zeros((128 - rows, pair_w), F32)], axis=0)).astype(BF16)

    scale = head ** -0.5
    lane_s = lax.broadcasted_iota(jnp.int32, (2 * head, seq), 1)
    sub_b = lax.broadcasted_iota(jnp.int32, (2 * head, seq), 0)
    lane_h = lax.broadcasted_iota(jnp.int32, (pairs, 2 * head), 1)

    batch = 8

    def attend_body(i, carry):
        bs = [i * batch + k for k in range(batch)]
        at = [pl.ds(pl.multiple_of(b * head, head), head) for b in bs]
        rr = [pl.ds(pl.multiple_of(b * pairs, pairs), pairs) for b in bs]
        k_old = [k_buf[r, :] for r in at]
        v_old = [v_buf[r, :] for r in at]
        q2 = [q_rows[r, :] for r in rr]
        pos = [pos_smem[0, b] for b in bs]
        pick = jnp.concatenate([jnp.where(sub_b == b, 1.0, 0.0).astype(BF16) for b in bs], axis=1)
        col = jnp.dot(new_kv[...], pick, preferred_element_type=F32)
        keys, vals, scores = [], [], []
        for k in range(batch):
            here = lane_s[0:head] == pos[k]
            c = col[:, k * seq:(k + 1) * seq]
            keys.append(jnp.where(here, c[0:head], k_old[k].astype(F32)).astype(BF16))
            vals.append(jnp.where(here, c[head:], v_old[k].astype(F32)).astype(BF16))
        for k in range(batch):
            q = jnp.concatenate([jnp.where(lane_h < head, q2[k], 0.0), jnp.where(lane_h < head, 0.0, q2[k])], axis=0).astype(BF16)
            s = jnp.dot(q, jnp.concatenate([keys[k], keys[k]], axis=0), preferred_element_type=F32) * scale
            scores.append(jnp.where(lane_s[0:2 * pairs] <= pos[k], s, NEG_BIG))
        top = [jnp.max(s, axis=1, keepdims=True) for s in scores]
        e = [jnp.exp(s - m) for s, m in zip(scores, top)]
        den = [jnp.sum(x, axis=1, keepdims=True) for x in e]
        p = [(x / d).astype(BF16) for x, d in zip(e, den)]
        o = [lax.dot_general(p[k], jnp.concatenate([vals[k], vals[k]], axis=0), (((1,), (1,)), ((), ())), preferred_element_type=F32) for k in range(batch)]
        for k in range(batch):
            ctx_rows[rr[k], :] = jnp.where(lane_h < head, o[k][0:pairs], o[k][pairs:])
        for k in range(batch):
            k_buf[at[k], :] = keys[k]
            v_buf[at[k], :] = vals[k]
        return carry

    with jax.named_scope('attend'):
        lax.fori_loop(0, rows // batch, attend_body, 0)
    for p in range(pairs):
        act[:, CHUNK + ff + p * 2 * head: CHUNK + ff + (p + 1) * 2 * head] = ctx_rows[pl.ds(p, rows, stride=pairs), :].astype(BF16)

    pre[...] = jnp.zeros_like(pre)

    def up_body(n, carry):
        @pl.when((n > 0) & (n + A_SLOTS - 1 < n_up))
        def _():
            start_up(n + A_SLOTS - 1)

        @pl.when(n + A_SLOTS - 1 == n_up)
        def _():
            for c in range(1, B_SLOTS):
                start_down(c)

        @pl.when(n + A_SLOTS - 1 >= n_up)
        def _():
            start_down(n + A_SLOTS - 1 - n_up + B_SLOTS)

        with jax.named_scope('up_wait'):
            wait_up(n)
        act[:, pl.ds(pl.multiple_of(n * CHUNK, CHUNK), CHUNK)] = gelu_exact(pre[...]).astype(BF16)
        pre[...] = jnp.dot(mlp_in[...], ring[pl.ds(pl.multiple_of(a_slot(n) * width, width), width), :], preferred_element_type=F32)
        return carry

    with jax.named_scope('up'):
        lax.fori_loop(0, n_up, up_body, 0)
    act[:, ff:ff + CHUNK] = gelu_exact(pre[...]).astype(BF16)

    n_paired = n_down - N_DIRECT
    my_rows = pl.ds(pl.multiple_of(core * half_rows, half_rows), half_rows)
    other_rows = pl.ds(pl.multiple_of((1 - core) * half_rows, half_rows), half_rows)

    def chunk_cols(c):
        return pl.ds(pl.multiple_of(c * CHUNK, CHUNK), CHUNK)

    def quarter_cols(c, q):
        return pl.ds(pl.multiple_of(c * CHUNK + q * quarter, quarter), quarter)

    def slot_cols(c):
        return pl.ds(pl.multiple_of(c * quarter, quarter), quarter)

    def send_pair(c):
        pltpu.make_async_remote_copy(src_ref=part_buf.at[other_rows, chunk_cols(c)], dst_ref=pair_in.at[:, chunk_cols(c)],
                                     send_sem=sem_sent.at[0], recv_sem=sem_pair.at[c],
                                     device_id={'tp': chip * 2 + 1 - core}, device_id_type=pl.DeviceIdType.MESH).start()

    def send_quarters(c):
        pltpu.make_async_copy(pair_in.at[:, chunk_cols(c)], pair_in.at[:, chunk_cols(c)], sem_pair.at[c]).wait()
        both = part_buf[my_rows, chunk_cols(c)].astype(F32) + pair_in[:, chunk_cols(c)].astype(F32)
        sum_buf[:, chunk_cols(c)] = both.astype(BF16)
        for d in sorted(range(1, n_chips), key=lambda d: -min(d, n_chips - d)):
            q = lax.rem(chip + d, n_chips)
            pltpu.make_async_remote_copy(src_ref=sum_buf.at[:, quarter_cols(c, q)], dst_ref=quarter_in.at[d - 1, :, slot_cols(c)],
                                         send_sem=sem_sent.at[1], recv_sem=sem_quarter.at[c],
                                         device_id={'tp': q * 2 + core}, device_id_type=pl.DeviceIdType.MESH).start()

    def send_result(c):
        total = x_buf[my_rows, quarter_cols(c, chip)].astype(F32) + sum_buf[:, quarter_cols(c, chip)].astype(F32)
        pltpu.make_async_copy(quarter_in.at[:, :, slot_cols(c)], quarter_in.at[:, :, slot_cols(c)], sem_quarter.at[c]).wait()
        for d in range(1, n_chips):
            total = total + quarter_in[d - 1, :, slot_cols(c)].astype(F32)
        gather(c, total)

    def gather(c, total):
        out_buf[my_rows, quarter_cols(c, chip)] = total.astype(BF16)
        for d in sorted(range(1, n_tp), key=lambda d: -min(d, n_tp - d)):
            pltpu.make_async_remote_copy(src_ref=out_buf.at[my_rows, quarter_cols(c, chip)], dst_ref=out_buf.at[my_rows, quarter_cols(c, chip)],
                                         send_sem=sem_sent.at[2], recv_sem=sem_gather.at[0],
                                         device_id={'tp': lax.rem(me + d, n_tp)}, device_id_type=pl.DeviceIdType.MESH).start()

    def send_direct(c):
        for d in sorted(range(1, n_tp), key=lambda d: -min(d, n_tp - d)):
            to = lax.rem(me + d, n_tp)
            src = part_buf.at[pl.ds(pl.multiple_of(lax.rem(to, 2) * half_rows, half_rows), half_rows), quarter_cols(c, to // 2)]
            pltpu.make_async_remote_copy(src_ref=src, dst_ref=last_in.at[c - n_paired, d - 1], send_sem=sem_sent.at[3], recv_sem=sem_last.at[c - n_paired],
                                         device_id={'tp': to}, device_id_type=pl.DeviceIdType.MESH).start()

    def send_result_direct(c):
        total = x_buf[my_rows, quarter_cols(c, chip)].astype(F32) + part_buf[my_rows, quarter_cols(c, chip)].astype(F32)
        pltpu.make_async_copy(last_in.at[c - n_paired], last_in.at[c - n_paired], sem_last.at[c - n_paired]).wait()
        for d in range(1, n_tp):
            total = total + last_in[c - n_paired, d - 1].astype(F32)
        gather(c, total)

    lag = 4
    pl.semaphore_wait(barrier, n_tp - 1)
    start_down(n_slots - 1)

    def multiply(c, groups):
        total = None
        for span in groups:
            with jax.named_scope('down_wait'):
                for i in span:
                    down_copy(c, i, sem_b.at[n_slots + i] if len(groups) > 1 else sem_b.at[lax.rem(c, n_slots)]).wait()
            first, count = parts[span[0]][0], sum(parts[i][1] for i in span)
            w = ring[pl.ds(down_base(c) + first, count), :]
            d = jnp.dot(act[:, CHUNK + first:CHUNK + first + count], w, preferred_element_type=F32)
            total = d if total is None else total + d
        part_buf[:, chunk_cols(c)] = total.astype(BF16)

    def down_body(c, carry):
        @pl.when((c > 0) & (c + n_slots < n_down))
        def _():
            start_down(c + n_slots - 1)

        @pl.when(c + n_slots == n_down)
        def _():
            start_last_down()

        multiply(c, ((0, 1, 2),))
        send_pair(c)

        @pl.when(c >= 1)
        def _():
            with jax.named_scope('quarters'):
                send_quarters(c - 1)

        @pl.when(c >= lag)
        def _():
            with jax.named_scope('result'):
                send_result(c - lag)

        return carry

    with jax.named_scope('down'):
        lax.fori_loop(0, n_paired, down_body, 0)
    done = n_paired - lag
    for c in range(n_paired, n_down):
        with jax.named_scope('tail_multiply'):
            multiply(c, ((0, 1, 2),) if c < n_down - 1 else ((0,), (1,), (2,)))
        send_direct(c)
        if c == n_paired:
            with jax.named_scope('tail_quarters'):
                send_quarters(c - 1)
        with jax.named_scope('tail_result'):
            send_result(done)
        done += 1
    for c in range(done, n_paired):
        with jax.named_scope('tail_result'):
            send_result(c)
    for c in range(n_paired, n_down):
        with jax.named_scope('tail_direct'):
            send_result_direct(c)

    def settle(sem, n_rows):
        pltpu.make_async_copy(out_buf.at[0:n_rows, :], out_buf.at[0:n_rows, :], sem).wait()

    with jax.named_scope('gather_wait'):
        settle(sem_gather.at[0], (n_tp - 1) * rows // n_tp)
    with jax.named_scope('sent_wait'):
        sent = pltpu.make_async_copy(part_buf.at[other_rows, 0:n_paired * CHUNK], part_buf.at[other_rows, 0:n_paired * CHUNK], sem_sent.at[0])
        sent.wait()
        for d in range(1, n_chips):
            pltpu.make_async_copy(quarter_in.at[d - 1, :, 0:n_paired * quarter], quarter_in.at[d - 1, :, 0:n_paired * quarter], sem_sent.at[1]).wait()
        settle(sem_sent.at[2], (n_tp - 1) * rows // n_tp)
        pltpu.make_async_copy(last_in, last_in, sem_sent.at[3]).wait()


def write_kernel(a_ref, b_ref, c_ref, a_out, b_out, c_out, sem):
    copies = []
    for i, (src, dst) in enumerate(((a_ref, a_out), (b_ref, b_out), (c_ref, c_out))):
        copies.append(pltpu.make_async_copy(src, dst, sem.at[i]))
    for c in copies:
        c.start()
    for c in copies:
        c.wait()


def solution(mesh):
    row_spec = P('dp', None)
    vec_spec = P(None)
    cache_spec = P('dp', 'tp', None, None)

    def device_step(x, ga, ba, gm, bm, w_qkv, w_out, w_up, w_down, k_cache, v_cache, positions):
        rows, width = x.shape
        ff = w_up.shape[1]
        n_query, head = w_qkv.shape[2] - 2, w_qkv.shape[3]
        seq = k_cache.shape[2]
        ctx_w = n_query * head
        qk_rows = (n_query + 2) * head
        n_qkv = width // CHUNK
        n_tp = mesh.shape['tp']
        n_chips = n_tp // 2
        n_down = width // CHUNK
        dims = (rows, width, ff, n_query, head, seq, n_tp)
        wq = jnp.transpose(w_qkv, (1, 2, 3, 0)).reshape(qk_rows, width)
        wo = w_out.reshape(ctx_w, width)
        kt = jnp.transpose(k_cache, (0, 1, 3, 2)).reshape(rows * head, seq)
        vt = jnp.transpose(v_cache, (0, 1, 3, 2)).reshape(rows * head, seq)
        any_spec = pl.BlockSpec(memory_space=pl.ANY)
        vmem_spec = pl.BlockSpec(memory_space=pltpu.VMEM)
        out, k_new, v_new = pl.pallas_call(
            lambda *refs: layer_kernel(dims, *refs),
            name='layer',
            out_shape=(pltpu.VMEM((rows, width), BF16), pltpu.VMEM(kt.shape, BF16), pltpu.VMEM(vt.shape, BF16)),
            in_specs=[any_spec] * 12,
            out_specs=(vmem_spec, vmem_spec, vmem_spec),
            scratch_shapes=[
                pltpu.VMEM((A_SLOTS * width + B_SLOTS * (ff + ctx_w), CHUNK), BF16),
                pltpu.VMEM((rows, width), BF16),
                pltpu.VMEM((rows, width), BF16),
                pltpu.VMEM((rows, width), BF16),
                pltpu.VMEM((rows, CHUNK + ff + ctx_w), BF16),
                pltpu.VMEM((rows, qk_rows), F32),
                pltpu.VMEM((2 * head, 128), BF16),
                pltpu.VMEM((rows * n_query // 2, 128), F32),
                pltpu.VMEM((rows * n_query // 2, 128), F32),
                pltpu.VMEM((rows, CHUNK), F32),
                pltpu.VMEM((4, width), F32),
                pltpu.VMEM((1, rows), jnp.int32),
                pltpu.SMEM((1, rows), jnp.int32),
                pltpu.VMEM((rows, width), BF16),
                pltpu.VMEM((rows // 2, width), BF16),
                pltpu.VMEM((rows // 2, width), BF16),
                pltpu.VMEM((n_chips - 1, rows // 2, width // n_chips), BF16),
                pltpu.VMEM((N_DIRECT, n_tp - 1, rows // 2, CHUNK // n_chips), BF16),
                pltpu.SemaphoreType.DMA((5,)),
                pltpu.SemaphoreType.DMA((n_qkv // QKV_GROUP,)),
                pltpu.SemaphoreType.DMA((A_SLOTS,)),
                pltpu.SemaphoreType.DMA((A_SLOTS + B_SLOTS + 3,)),
                pltpu.SemaphoreType.DMA((n_down - N_DIRECT,)),
                pltpu.SemaphoreType.DMA((n_down - N_DIRECT,)),
                pltpu.SemaphoreType.DMA((1,)),
                pltpu.SemaphoreType.DMA((N_DIRECT,)),
                pltpu.SemaphoreType.DMA((4,)),
            ],
            compiler_params=pltpu.CompilerParams(vmem_limit_bytes=60 * 1024 * 1024, collective_id=0, has_side_effects=True),
        )(x, ga.reshape(1, width), ba.reshape(1, width), gm.reshape(1, width), bm.reshape(1, width), wq, wo, w_up, w_down, kt, vt, positions.reshape(1, rows))
        out, k_new, v_new = (pltpu.with_memory_space_constraint(v, pltpu.VMEM) for v in (out, k_new, v_new))
        out, k_new, v_new = pl.pallas_call(
            write_kernel,
            name='write',
            out_shape=(jax.ShapeDtypeStruct((rows, width), BF16), jax.ShapeDtypeStruct(kt.shape, BF16), jax.ShapeDtypeStruct(vt.shape, BF16)),
            in_specs=[vmem_spec] * 3,
            out_specs=(any_spec, any_spec, any_spec),
            scratch_shapes=[pltpu.SemaphoreType.DMA((3,))],
            compiler_params=pltpu.CompilerParams(vmem_limit_bytes=1024 * 1024),
        )(out, k_new, v_new)
        k_new = jnp.transpose(k_new.reshape(rows, 1, head, seq), (0, 1, 3, 2))
        v_new = jnp.transpose(v_new.reshape(rows, 1, head, seq), (0, 1, 3, 2))
        return out, k_new, v_new

    return jax.shard_map(device_step, mesh=mesh, in_specs=(row_spec, vec_spec, vec_spec, vec_spec, vec_spec, P(None, 'tp', None, None), P('tp', None, None, None), P(None, 'tp'), P('tp', None), cache_spec, cache_spec, P('dp')), out_specs=(row_spec, cache_spec, cache_spec), check_vma=False)
```

```python
import math
import numpy as np
import jax
import jax.numpy as jnp
from jax import lax
from jax.experimental import pallas as pl
from jax.experimental.pallas import tpu as pltpu
from jax.sharding import PartitionSpec as P

LN_EPS = 1e-5
ROPE_BASE = 10000.0
NEG_BIG = -1e30
F32 = jnp.float32
BF16 = jnp.bfloat16
CHUNK = 512
A_SLOTS = 4
B_SLOTS = 3
N_DIRECT = 2
PAIR_SEMS = 4
QUARTER_SEMS = 8
QKV_GROUP = 4


def gelu_exact(pre):
    return pre * 0.5 * (1.0 + lax.erf(pre * (1.0 / math.sqrt(2.0))))


def layer_kernel(dims, x_hbm, ga_hbm, ba_hbm, gm_hbm, bm_hbm, wqkv_hbm, wout_hbm, wup_hbm, wdown_hbm, kc_hbm, vc_hbm, pos_hbm,
                 out_buf, k_buf, v_buf,
                 ring, x_buf, attn_in, mlp_in, act, qkv_acc, new_kv, q_rows, ctx_rows, pre, vecs, pos_vec, pos_smem, part_buf, pair_in, sum_buf, quarter_in, last_in,
                 sem_in, sem_qkv, sem_a, sem_b, sem_pair, sem_quarter, sem_gather, sem_last, sem_sent):
    rows, width, ff, n_query, head, seq, n_tp = dims
    qk_rows = (n_query + 2) * head
    n_qkv = width // CHUNK
    n_up = ff // CHUNK
    n_down = width // CHUNK
    ctx_w = n_query * head
    pairs = n_query // 2
    per_slot = width // qk_rows
    group = QKV_GROUP

    def qkv_row(j):
        return (j // per_slot) * width + (j % per_slot) * qk_rows

    def small_copies():
        return [
            pltpu.make_async_copy(x_hbm, x_buf, sem_in.at[0]),
            pltpu.make_async_copy(ga_hbm, vecs.at[0:1], sem_in.at[0]),
            pltpu.make_async_copy(ba_hbm, vecs.at[1:2], sem_in.at[0]),
            pltpu.make_async_copy(gm_hbm, vecs.at[2:3], sem_in.at[0]),
            pltpu.make_async_copy(bm_hbm, vecs.at[3:4], sem_in.at[0]),
            pltpu.make_async_copy(pos_hbm, pos_vec, sem_in.at[1]),
            pltpu.make_async_copy(pos_hbm, pos_smem, sem_in.at[1]),
            pltpu.make_async_copy(kc_hbm, k_buf, sem_in.at[1]),
            pltpu.make_async_copy(vc_hbm, v_buf, sem_in.at[1]),
        ]

    def qkv_copy(j):
        return pltpu.make_async_copy(wqkv_hbm.at[:, pl.ds(j * CHUNK, CHUNK)], ring.at[pl.ds(qkv_row(j), qk_rows), :], sem_qkv.at[j // group])

    def a_slot(n):
        return lax.rem(n + 3, A_SLOTS)

    def start_up(n):
        part = width // 4
        base = a_slot(n) * width
        for i in range(4):
            pltpu.make_async_copy(wup_hbm.at[pl.ds(i * part, part), pl.ds(pl.multiple_of(n * CHUNK, CHUNK), CHUNK)],
                                  ring.at[pl.ds(base + i * part, part), :], sem_a.at[a_slot(n)]).start()

    def wait_up(n):
        pltpu.make_async_copy(wup_hbm.at[:, pl.ds(pl.multiple_of(n * CHUNK, CHUNK), CHUNK)],
                              ring.at[pl.ds(a_slot(n) * width, width), :], sem_a.at[a_slot(n)]).wait()

    b_rows = ff + ctx_w
    n_slots = A_SLOTS + B_SLOTS
    parts = ((0, ff // 2), (ff // 2, ff // 2), (ff, ctx_w))

    def down_base(c):
        s = lax.rem(c, n_slots)
        large = lax.rem(a_slot(n_up - A_SLOTS) + s - B_SLOTS + A_SLOTS, A_SLOTS) * width
        return pl.multiple_of(jnp.where(s < B_SLOTS, A_SLOTS * width + s * b_rows, large), 1024)

    def down_copy(c, i, sem):
        first, count = parts[i]
        cols = pl.ds(pl.multiple_of(c * CHUNK, CHUNK), CHUNK)
        src = wout_hbm.at[:, cols] if i == 2 else wdown_hbm.at[pl.ds(first, count), cols]
        return pltpu.make_async_copy(src, ring.at[pl.ds(down_base(c) + first, count), :], sem)

    def start_down(c):
        for i in range(len(parts)):
            down_copy(c, i, sem_b.at[lax.rem(c, n_slots)]).start()

    def start_last_down():
        for i in range(len(parts)):
            down_copy(n_down - 1, i, sem_b.at[n_slots + i]).start()

    small = small_copies()
    for c in small[:7]:
        c.start()

    me = lax.axis_index('tp')
    n_chips = n_tp // 2
    chip, core = me // 2, lax.rem(me, 2)
    half_rows = rows // 2
    quarter = CHUNK // n_chips
    barrier = pltpu.get_barrier_semaphore()
    for d in range(1, n_tp):
        pl.semaphore_signal(barrier, inc=1, device_id={'tp': lax.rem(me + d, n_tp)}, device_id_type=pl.DeviceIdType.MESH)
    for j in range(n_qkv):
        qkv_copy(j).start()

    for c in small[:5]:
        c.wait()
    lanes = 512
    n_l = width // lanes

    def fold(v):
        t = v[:, 0:128]
        for i in range(1, lanes // 128):
            t = t + v[:, i * 128:(i + 1) * 128]
        return t

    def sum_body(j, acc):
        return acc + fold(x_buf[:, pl.ds(pl.multiple_of(j * lanes, lanes), lanes)].astype(F32))

    total = lax.fori_loop(0, n_l, sum_body, jnp.zeros((rows, 128), F32))
    mean = jnp.sum(total, axis=1, keepdims=True) * (1.0 / width)

    def var_body(j, acc):
        d = x_buf[:, pl.ds(pl.multiple_of(j * lanes, lanes), lanes)].astype(F32) - mean
        return acc + fold(d * d)

    total2 = lax.fori_loop(0, n_l, var_body, jnp.zeros((rows, 128), F32))
    rstd = lax.rsqrt(jnp.sum(total2, axis=1, keepdims=True) * (1.0 / width) + LN_EPS)

    def norm_body(j, carry):
        cols = pl.ds(pl.multiple_of(j * lanes, lanes), lanes)
        nrm = (x_buf[:, cols].astype(F32) - mean) * rstd
        attn_in[0:rows, cols] = (nrm * vecs[0:1, cols] + vecs[1:2, cols]).astype(BF16)
        mlp_in[:, cols] = (nrm * vecs[2:3, cols] + vecs[3:4, cols]).astype(BF16)
        return carry

    with jax.named_scope('norm'):
        lax.fori_loop(0, n_l, norm_body, 0)


    def qkv_step(g):
        tot = None
        with jax.named_scope('qkv_wait'):
            for i in range(group):
                qkv_copy(g * group + i).wait()
        for i in range(group):
            j = g * group + i
            w = ring[qkv_row(j):qkv_row(j) + qk_rows, :]
            a = attn_in[:, j * CHUNK:(j + 1) * CHUNK]
            d = lax.dot_general(a, w, (((1,), (1,)), ((), ())), preferred_element_type=F32)
            tot = d if tot is None else tot + d

        qkv_acc[...] = tot if g == 0 else qkv_acc[...] + tot

    for g in range(n_qkv // group):
        if g == 0:
            small[7].start()
            small[8].start()
            start_up(0)
        if g == 2:
            start_up(1)
        with jax.named_scope('qkv'):
            qkv_step(g)
    for n in range(2, A_SLOTS):
        start_up(n)
    start_down(0)

    for c in small[5:]:
        c.wait()
    half = head // 2
    pair_w = 2 * head
    pos_row = jnp.concatenate([pos_vec[...], pos_vec[...]], axis=1).astype(F32)
    pos_col = jnp.transpose(jnp.broadcast_to(pos_row, (128, 128)))[0:rows, :]
    lane = lax.broadcasted_iota(jnp.int32, (rows, pair_w), 1)
    first_half = lax.rem(lane, head) < half
    angles = jnp.exp(lax.rem(lane, half).astype(F32) * (-2.0 * math.log(ROPE_BASE) / head)) * pos_col
    cos_t = jnp.cos(angles)
    sin_t = jnp.where(first_half, -jnp.sin(angles), jnp.sin(angles))

    def rotate(u):
        swapped = jnp.where(first_half, pltpu.roll(u, pair_w - half, axis=1), pltpu.roll(u, half, axis=1))
        return u * cos_t + swapped * sin_t

    for p in range(pairs):
        q_rows[pl.ds(p, rows, stride=pairs), :] = rotate(qkv_acc[:, p * pair_w:(p + 1) * pair_w].astype(BF16).astype(F32))
    kv = qkv_acc[:, pairs * pair_w:].astype(BF16).astype(F32)
    kv = jnp.where(lane < head, rotate(kv), kv)
    new_kv[...] = jnp.transpose(jnp.concatenate([kv, jnp.zeros((128 - rows, pair_w), F32)], axis=0)).astype(BF16)

    scale = head ** -0.5
    lane_s = lax.broadcasted_iota(jnp.int32, (2 * head, seq), 1)
    sub_b = lax.broadcasted_iota(jnp.int32, (2 * head, seq), 0)
    lane_h = lax.broadcasted_iota(jnp.int32, (pairs, 2 * head), 1)

    batch = 8

    def attend_body(i, carry):
        bs = [i * batch + k for k in range(batch)]
        at = [pl.ds(pl.multiple_of(b * head, head), head) for b in bs]
        rr = [pl.ds(pl.multiple_of(b * pairs, pairs), pairs) for b in bs]
        k_old = [k_buf[r, :] for r in at]
        v_old = [v_buf[r, :] for r in at]
        q2 = [q_rows[r, :] for r in rr]
        pos = [pos_smem[0, b] for b in bs]
        pick = jnp.concatenate([jnp.where(sub_b == b, 1.0, 0.0).astype(BF16) for b in bs], axis=1)
        col = jnp.dot(new_kv[...], pick, preferred_element_type=F32)
        keys, vals, scores = [], [], []
        for k in range(batch):
            here = lane_s[0:head] == pos[k]
            c = col[:, k * seq:(k + 1) * seq]
            keys.append(jnp.where(here, c[0:head], k_old[k].astype(F32)).astype(BF16))
            vals.append(jnp.where(here, c[head:], v_old[k].astype(F32)).astype(BF16))
        for k in range(batch):
            q = jnp.concatenate([jnp.where(lane_h < head, q2[k], 0.0), jnp.where(lane_h < head, 0.0, q2[k])], axis=0).astype(BF16)
            s = jnp.dot(q, jnp.concatenate([keys[k], keys[k]], axis=0), preferred_element_type=F32) * scale
            scores.append(jnp.where(lane_s[0:2 * pairs] <= pos[k], s, NEG_BIG))
        top = [jnp.max(s, axis=1, keepdims=True) for s in scores]
        e = [jnp.exp(s - m) for s, m in zip(scores, top)]
        den = [jnp.sum(x, axis=1, keepdims=True) for x in e]
        p = [(x / d).astype(BF16) for x, d in zip(e, den)]
        o = [lax.dot_general(p[k], jnp.concatenate([vals[k], vals[k]], axis=0), (((1,), (1,)), ((), ())), preferred_element_type=F32) for k in range(batch)]
        for k in range(batch):
            ctx_rows[rr[k], :] = jnp.where(lane_h < head, o[k][0:pairs], o[k][pairs:])
        for k in range(batch):
            k_buf[at[k], :] = keys[k]
            v_buf[at[k], :] = vals[k]
        return carry

    with jax.named_scope('attend'):
        lax.fori_loop(0, rows // batch, attend_body, 0)
    for p in range(pairs):
        act[:, CHUNK + ff + p * 2 * head: CHUNK + ff + (p + 1) * 2 * head] = ctx_rows[pl.ds(p, rows, stride=pairs), :].astype(BF16)

    pre[...] = jnp.zeros_like(pre)

    def up_body(n, carry):
        @pl.when((n > 0) & (n + A_SLOTS - 1 < n_up))
        def _():
            start_up(n + A_SLOTS - 1)

        @pl.when(n + A_SLOTS - 1 == n_up)
        def _():
            for c in range(1, B_SLOTS):
                start_down(c)

        @pl.when(n + A_SLOTS - 1 >= n_up)
        def _():
            start_down(n + A_SLOTS - 1 - n_up + B_SLOTS)

        with jax.named_scope('up_wait'):
            wait_up(n)
        act[:, pl.ds(pl.multiple_of(n * CHUNK, CHUNK), CHUNK)] = gelu_exact(pre[...]).astype(BF16)
        pre[...] = jnp.dot(mlp_in[...], ring[pl.ds(pl.multiple_of(a_slot(n) * width, width), width), :], preferred_element_type=F32)
        return carry

    with jax.named_scope('up'):
        lax.fori_loop(0, n_up, up_body, 0)
    act[:, ff:ff + CHUNK] = gelu_exact(pre[...]).astype(BF16)

    n_paired = n_down - N_DIRECT
    my_rows = pl.ds(pl.multiple_of(core * half_rows, half_rows), half_rows)
    other_rows = pl.ds(pl.multiple_of((1 - core) * half_rows, half_rows), half_rows)

    def chunk_cols(c):
        return pl.ds(pl.multiple_of(c * CHUNK, CHUNK), CHUNK)

    def quarter_cols(c, q):
        return pl.ds(pl.multiple_of(c * CHUNK + q * quarter, quarter), quarter)

    def slot_cols(c):
        return pl.ds(pl.multiple_of(c * quarter, quarter), quarter)

    def send_pair(c):
        pltpu.make_async_remote_copy(src_ref=part_buf.at[other_rows, chunk_cols(c)], dst_ref=pair_in.at[:, chunk_cols(c)],
                                     send_sem=sem_sent.at[0], recv_sem=sem_pair.at[lax.rem(c, PAIR_SEMS)],
                                     device_id={'tp': chip * 2 + 1 - core}, device_id_type=pl.DeviceIdType.MESH).start()

    def send_quarters(c):
        pltpu.make_async_copy(pair_in.at[:, chunk_cols(c)], pair_in.at[:, chunk_cols(c)], sem_pair.at[lax.rem(c, PAIR_SEMS)]).wait()
        both = part_buf[my_rows, chunk_cols(c)].astype(F32) + pair_in[:, chunk_cols(c)].astype(F32)
        sum_buf[:, chunk_cols(c)] = both.astype(BF16)
        for d in sorted(range(1, n_chips), key=lambda d: -min(d, n_chips - d)):
            q = lax.rem(chip + d, n_chips)
            pltpu.make_async_remote_copy(src_ref=sum_buf.at[:, quarter_cols(c, q)], dst_ref=quarter_in.at[d - 1, :, slot_cols(c)],
                                         send_sem=sem_sent.at[0], recv_sem=sem_quarter.at[lax.rem(c, QUARTER_SEMS)],
                                         device_id={'tp': q * 2 + core}, device_id_type=pl.DeviceIdType.MESH).start()

    def send_result(c):
        total = x_buf[my_rows, quarter_cols(c, chip)].astype(F32) + sum_buf[:, quarter_cols(c, chip)].astype(F32)
        pltpu.make_async_copy(quarter_in.at[:, :, slot_cols(c)], quarter_in.at[:, :, slot_cols(c)], sem_quarter.at[lax.rem(c, QUARTER_SEMS)]).wait()
        for d in range(1, n_chips):
            total = total + quarter_in[d - 1, :, slot_cols(c)].astype(F32)
        gather(c, total)

    def gather(c, total):
        out_buf[my_rows, quarter_cols(c, chip)] = total.astype(BF16)
        for d in sorted(range(1, n_tp), key=lambda d: -min(d, n_tp - d)):
            pltpu.make_async_remote_copy(src_ref=out_buf.at[my_rows, quarter_cols(c, chip)], dst_ref=out_buf.at[my_rows, quarter_cols(c, chip)],
                                         send_sem=sem_sent.at[0], recv_sem=sem_gather.at[0],
                                         device_id={'tp': lax.rem(me + d, n_tp)}, device_id_type=pl.DeviceIdType.MESH).start()

    def send_direct(c):
        for d in sorted(range(1, n_tp), key=lambda d: -min(d, n_tp - d)):
            to = lax.rem(me + d, n_tp)
            src = part_buf.at[pl.ds(pl.multiple_of(lax.rem(to, 2) * half_rows, half_rows), half_rows), quarter_cols(c, to // 2)]
            pltpu.make_async_remote_copy(src_ref=src, dst_ref=last_in.at[c - n_paired, d - 1], send_sem=sem_sent.at[0], recv_sem=sem_last.at[c - n_paired],
                                         device_id={'tp': to}, device_id_type=pl.DeviceIdType.MESH).start()

    def send_result_direct(c):
        total = x_buf[my_rows, quarter_cols(c, chip)].astype(F32) + part_buf[my_rows, quarter_cols(c, chip)].astype(F32)
        pltpu.make_async_copy(last_in.at[c - n_paired], last_in.at[c - n_paired], sem_last.at[c - n_paired]).wait()
        for d in range(1, n_tp):
            total = total + last_in[c - n_paired, d - 1].astype(F32)
        gather(c, total)

    lag = 4
    pl.semaphore_wait(barrier, n_tp - 1)
    start_down(n_slots - 1)

    def multiply(c, groups):
        total = None
        for span in groups:
            with jax.named_scope('down_wait'):
                for i in span:
                    down_copy(c, i, sem_b.at[n_slots + i] if len(groups) > 1 else sem_b.at[lax.rem(c, n_slots)]).wait()
            first, count = parts[span[0]][0], sum(parts[i][1] for i in span)
            w = ring[pl.ds(down_base(c) + first, count), :]
            d = jnp.dot(act[:, CHUNK + first:CHUNK + first + count], w, preferred_element_type=F32)
            total = d if total is None else total + d
        part_buf[:, chunk_cols(c)] = total.astype(BF16)

    def down_body(c, carry):
        @pl.when((c > 0) & (c + n_slots < n_down))
        def _():
            start_down(c + n_slots - 1)

        @pl.when(c + n_slots == n_down)
        def _():
            start_last_down()

        multiply(c, ((0, 1, 2),))
        send_pair(c)

        @pl.when(c >= 1)
        def _():
            with jax.named_scope('quarters'):
                send_quarters(c - 1)

        @pl.when(c >= lag)
        def _():
            with jax.named_scope('result'):
                send_result(c - lag)

        return carry

    with jax.named_scope('down'):
        lax.fori_loop(0, n_paired, down_body, 0)
    done = n_paired - lag
    for c in range(n_paired, n_down):
        with jax.named_scope('tail_multiply'):
            multiply(c, ((0, 1, 2),) if c < n_down - 1 else ((0,), (1,), (2,)))
        send_direct(c)
        if c == n_paired:
            with jax.named_scope('tail_quarters'):
                send_quarters(c - 1)
        with jax.named_scope('tail_result'):
            send_result(done)
        done += 1
    for c in range(done, n_paired):
        with jax.named_scope('tail_result'):
            send_result(c)
    for c in range(n_paired, n_down):
        with jax.named_scope('tail_direct'):
            send_result_direct(c)

    def settle(sem, n_rows):
        pltpu.make_async_copy(out_buf.at[0:n_rows, :], out_buf.at[0:n_rows, :], sem).wait()

    with jax.named_scope('gather_wait'):
        settle(sem_gather.at[0], (n_tp - 1) * rows // n_tp)
    with jax.named_scope('sent_wait'):
        sent = pltpu.make_async_copy(part_buf.at[other_rows, 0:n_paired * CHUNK], part_buf.at[other_rows, 0:n_paired * CHUNK], sem_sent.at[0])
        sent.wait()
        for d in range(1, n_chips):
            pltpu.make_async_copy(quarter_in.at[d - 1, :, 0:n_paired * quarter], quarter_in.at[d - 1, :, 0:n_paired * quarter], sem_sent.at[0]).wait()
        settle(sem_sent.at[0], (n_tp - 1) * rows // n_tp)
        pltpu.make_async_copy(last_in, last_in, sem_sent.at[0]).wait()


def write_kernel(a_ref, b_ref, c_ref, a_out, b_out, c_out, sem):
    copies = []
    for i, (src, dst) in enumerate(((a_ref, a_out), (b_ref, b_out), (c_ref, c_out))):
        copies.append(pltpu.make_async_copy(src, dst, sem.at[i]))
    for c in copies:
        c.start()
    for c in copies:
        c.wait()


def solution(mesh):
    row_spec = P('dp', None)
    vec_spec = P(None)
    cache_spec = P('dp', 'tp', None, None)

    def device_step(x, ga, ba, gm, bm, w_qkv, w_out, w_up, w_down, k_cache, v_cache, positions):
        rows, width = x.shape
        ff = w_up.shape[1]
        n_query, head = w_qkv.shape[2] - 2, w_qkv.shape[3]
        seq = k_cache.shape[2]
        ctx_w = n_query * head
        qk_rows = (n_query + 2) * head
        n_qkv = width // CHUNK
        n_tp = mesh.shape['tp']
        n_chips = n_tp // 2
        n_down = width // CHUNK
        dims = (rows, width, ff, n_query, head, seq, n_tp)
        wq = jnp.transpose(w_qkv, (1, 2, 3, 0)).reshape(qk_rows, width)
        wo = w_out.reshape(ctx_w, width)
        kt = jnp.transpose(k_cache, (0, 1, 3, 2)).reshape(rows * head, seq)
        vt = jnp.transpose(v_cache, (0, 1, 3, 2)).reshape(rows * head, seq)
        any_spec = pl.BlockSpec(memory_space=pl.ANY)
        vmem_spec = pl.BlockSpec(memory_space=pltpu.VMEM)
        out, k_new, v_new = pl.pallas_call(
            lambda *refs: layer_kernel(dims, *refs),
            name='layer',
            out_shape=(pltpu.VMEM((rows, width), BF16), pltpu.VMEM(kt.shape, BF16), pltpu.VMEM(vt.shape, BF16)),
            in_specs=[any_spec] * 12,
            out_specs=(vmem_spec, vmem_spec, vmem_spec),
            scratch_shapes=[
                pltpu.VMEM((A_SLOTS * width + B_SLOTS * (ff + ctx_w), CHUNK), BF16),
                pltpu.VMEM((rows, width), BF16),
                pltpu.VMEM((rows, width), BF16),
                pltpu.VMEM((rows, width), BF16),
                pltpu.VMEM((rows, CHUNK + ff + ctx_w), BF16),
                pltpu.VMEM((rows, qk_rows), F32),
                pltpu.VMEM((2 * head, 128), BF16),
                pltpu.VMEM((rows * n_query // 2, 128), F32),
                pltpu.VMEM((rows * n_query // 2, 128), F32),
                pltpu.VMEM((rows, CHUNK), F32),
                pltpu.VMEM((4, width), F32),
                pltpu.VMEM((1, rows), jnp.int32),
                pltpu.SMEM((1, rows), jnp.int32),
                pltpu.VMEM((rows, width), BF16),
                pltpu.VMEM((rows // 2, width), BF16),
                pltpu.VMEM((rows // 2, width), BF16),
                pltpu.VMEM((n_chips - 1, rows // 2, width // n_chips), BF16),
                pltpu.VMEM((N_DIRECT, n_tp - 1, rows // 2, CHUNK // n_chips), BF16),
                pltpu.SemaphoreType.DMA((2,)),
                pltpu.SemaphoreType.DMA((n_qkv // QKV_GROUP,)),
                pltpu.SemaphoreType.DMA((A_SLOTS,)),
                pltpu.SemaphoreType.DMA((A_SLOTS + B_SLOTS + 3,)),
                pltpu.SemaphoreType.DMA((PAIR_SEMS,)),
                pltpu.SemaphoreType.DMA((QUARTER_SEMS,)),
                pltpu.SemaphoreType.DMA((1,)),
                pltpu.SemaphoreType.DMA((N_DIRECT,)),
                pltpu.SemaphoreType.DMA((1,)),
            ],
            compiler_params=pltpu.CompilerParams(vmem_limit_bytes=60 * 1024 * 1024, collective_id=0, has_side_effects=True),
        )(x, ga.reshape(1, width), ba.reshape(1, width), gm.reshape(1, width), bm.reshape(1, width), wq, wo, w_up, w_down, kt, vt, positions.reshape(1, rows))
        out, k_new, v_new = (pltpu.with_memory_space_constraint(v, pltpu.VMEM) for v in (out, k_new, v_new))
        out, k_new, v_new = pl.pallas_call(
            write_kernel,
            name='write',
            out_shape=(jax.ShapeDtypeStruct((rows, width), BF16), jax.ShapeDtypeStruct(kt.shape, BF16), jax.ShapeDtypeStruct(vt.shape, BF16)),
            in_specs=[vmem_spec] * 3,
            out_specs=(any_spec, any_spec, any_spec),
            scratch_shapes=[pltpu.SemaphoreType.DMA((3,))],
            compiler_params=pltpu.CompilerParams(vmem_limit_bytes=1024 * 1024),
        )(out, k_new, v_new)
        k_new = jnp.transpose(k_new.reshape(rows, 1, head, seq), (0, 1, 3, 2))
        v_new = jnp.transpose(v_new.reshape(rows, 1, head, seq), (0, 1, 3, 2))
        return out, k_new, v_new

    return jax.shard_map(device_step, mesh=mesh, in_specs=(row_spec, vec_spec, vec_spec, vec_spec, vec_spec, P(None, 'tp', None, None), P('tp', None, None, None), P(None, 'tp'), P('tp', None), cache_spec, cache_spec, P('dp')), out_specs=(row_spec, cache_spec, cache_spec), check_vma=False)
```

```python
import math
import numpy as np
import jax
import jax.numpy as jnp
from jax import lax
from jax.experimental import pallas as pl
from jax.experimental.pallas import tpu as pltpu
from jax.sharding import PartitionSpec as P

LN_EPS = 1e-5
ROPE_BASE = 10000.0
NEG_BIG = -1e30
F32 = jnp.float32
BF16 = jnp.bfloat16
CHUNK = 512
A_SLOTS = 4
B_SLOTS = 3
N_DIRECT = 2
PAIR_SEMS = 4
QUARTER_SEMS = 8
QKV_GROUP = 4


def gelu_exact(pre):
    return pre * 0.5 * (1.0 + lax.erf(pre * (1.0 / math.sqrt(2.0))))


def layer_kernel(dims, x_hbm, ga_hbm, ba_hbm, gm_hbm, bm_hbm, wqkv_hbm, wout_hbm, wup_hbm, wdown_hbm, kc_hbm, vc_hbm, pos_hbm,
                 out_buf, k_buf, v_buf,
                 ring, x_buf, attn_in, mlp_in, act, qkv_acc, new_kv, q_rows, ctx_rows, pre, vecs, pos_vec, pos_smem, part_buf, pair_in, sum_buf, quarter_in, last_in,
                 sem_in, sem_qkv, sem_a, sem_b, sem_pair, sem_quarter, sem_gather, sem_last, sem_sent):
    rows, width, ff, n_query, head, seq, n_tp = dims
    qk_rows = (n_query + 2) * head
    n_qkv = width // CHUNK
    n_up = ff // CHUNK
    n_down = width // CHUNK
    ctx_w = n_query * head
    pairs = n_query // 2
    per_slot = width // qk_rows
    group = QKV_GROUP

    def qkv_row(j):
        return (j // per_slot) * width + (j % per_slot) * qk_rows

    def small_copies():
        return [
            pltpu.make_async_copy(x_hbm, x_buf, sem_in.at[0]),
            pltpu.make_async_copy(ga_hbm, vecs.at[0:1], sem_in.at[0]),
            pltpu.make_async_copy(ba_hbm, vecs.at[1:2], sem_in.at[0]),
            pltpu.make_async_copy(gm_hbm, vecs.at[2:3], sem_in.at[0]),
            pltpu.make_async_copy(bm_hbm, vecs.at[3:4], sem_in.at[0]),
            pltpu.make_async_copy(pos_hbm, pos_vec, sem_in.at[1]),
            pltpu.make_async_copy(pos_hbm, pos_smem, sem_in.at[1]),
            pltpu.make_async_copy(kc_hbm, k_buf, sem_in.at[1]),
            pltpu.make_async_copy(vc_hbm, v_buf, sem_in.at[1]),
        ]

    def qkv_copy(j):
        return pltpu.make_async_copy(wqkv_hbm.at[:, pl.ds(j * CHUNK, CHUNK)], ring.at[pl.ds(qkv_row(j), qk_rows), :], sem_qkv.at[j // group])

    def a_slot(n):
        return lax.rem(n + 3, A_SLOTS)

    def start_up(n):
        part = width // 4
        base = a_slot(n) * width
        for i in range(4):
            pltpu.make_async_copy(wup_hbm.at[pl.ds(i * part, part), pl.ds(pl.multiple_of(n * CHUNK, CHUNK), CHUNK)],
                                  ring.at[pl.ds(base + i * part, part), :], sem_a.at[a_slot(n)]).start()

    def wait_up(n):
        pltpu.make_async_copy(wup_hbm.at[:, pl.ds(pl.multiple_of(n * CHUNK, CHUNK), CHUNK)],
                              ring.at[pl.ds(a_slot(n) * width, width), :], sem_a.at[a_slot(n)]).wait()

    b_rows = ff + ctx_w
    n_slots = A_SLOTS + B_SLOTS
    parts = ((0, ff // 2), (ff // 2, ff // 2), (ff, ctx_w))

    def down_base(c):
        s = lax.rem(c, n_slots)
        large = lax.rem(a_slot(n_up - A_SLOTS) + s - B_SLOTS + A_SLOTS, A_SLOTS) * width
        return pl.multiple_of(jnp.where(s < B_SLOTS, A_SLOTS * width + s * b_rows, large), 1024)

    def down_copy(c, i, sem):
        first, count = parts[i]
        cols = pl.ds(pl.multiple_of(c * CHUNK, CHUNK), CHUNK)
        src = wout_hbm.at[:, cols] if i == 2 else wdown_hbm.at[pl.ds(first, count), cols]
        return pltpu.make_async_copy(src, ring.at[pl.ds(down_base(c) + first, count), :], sem)

    def start_down(c):
        for i in range(len(parts)):
            down_copy(c, i, sem_b.at[lax.rem(c, n_slots)]).start()

    def start_last_down():
        for i in range(len(parts)):
            down_copy(n_down - 1, i, sem_b.at[n_slots + i]).start()

    small = small_copies()
    for c in small[:7]:
        c.start()

    me = lax.axis_index('tp')
    n_chips = n_tp // 2
    chip, core = me // 2, lax.rem(me, 2)
    half_rows = rows // 2
    quarter = CHUNK // n_chips
    barrier = pltpu.get_barrier_semaphore()
    for d in range(1, n_tp):
        pl.semaphore_signal(barrier, inc=1, device_id={'tp': lax.rem(me + d, n_tp)}, device_id_type=pl.DeviceIdType.MESH)
    for j in range(n_qkv):
        qkv_copy(j).start()

    for c in small[:5]:
        c.wait()
    lanes = 512
    n_l = width // lanes

    def fold(v):
        t = v[:, 0:128]
        for i in range(1, lanes // 128):
            t = t + v[:, i * 128:(i + 1) * 128]
        return t

    def sum_body(j, acc):
        return acc + fold(x_buf[:, pl.ds(pl.multiple_of(j * lanes, lanes), lanes)].astype(F32))

    total = lax.fori_loop(0, n_l, sum_body, jnp.zeros((rows, 128), F32))
    mean = jnp.sum(total, axis=1, keepdims=True) * (1.0 / width)

    def var_body(j, acc):
        d = x_buf[:, pl.ds(pl.multiple_of(j * lanes, lanes), lanes)].astype(F32) - mean
        return acc + fold(d * d)

    total2 = lax.fori_loop(0, n_l, var_body, jnp.zeros((rows, 128), F32))
    rstd = lax.rsqrt(jnp.sum(total2, axis=1, keepdims=True) * (1.0 / width) + LN_EPS)

    def norm_body(j, carry):
        cols = pl.ds(pl.multiple_of(j * lanes, lanes), lanes)
        nrm = (x_buf[:, cols].astype(F32) - mean) * rstd
        attn_in[0:rows, cols] = (nrm * vecs[0:1, cols] + vecs[1:2, cols]).astype(BF16)
        mlp_in[:, cols] = (nrm * vecs[2:3, cols] + vecs[3:4, cols]).astype(BF16)
        return carry

    with jax.named_scope('norm'):
        lax.fori_loop(0, n_l, norm_body, 0)


    def qkv_step(g):
        tot = None
        with jax.named_scope('qkv_wait'):
            for i in range(group):
                qkv_copy(g * group + i).wait()
        for i in range(group):
            j = g * group + i
            w = ring[qkv_row(j):qkv_row(j) + qk_rows, :]
            a = attn_in[:, j * CHUNK:(j + 1) * CHUNK]
            d = lax.dot_general(a, w, (((1,), (1,)), ((), ())), preferred_element_type=F32)
            tot = d if tot is None else tot + d

        qkv_acc[...] = tot if g == 0 else qkv_acc[...] + tot

    for g in range(n_qkv // group):
        if g == 0:
            small[7].start()
            small[8].start()
            start_up(0)
        if g == 2:
            start_up(1)
        with jax.named_scope('qkv'):
            qkv_step(g)
    for n in range(2, A_SLOTS):
        start_up(n)
    start_down(0)

    for c in small[5:]:
        c.wait()
    half = head // 2
    pair_w = 2 * head
    pos_row = jnp.concatenate([pos_vec[...], pos_vec[...]], axis=1).astype(F32)
    pos_col = jnp.transpose(jnp.broadcast_to(pos_row, (128, 128)))[0:rows, :]
    lane = lax.broadcasted_iota(jnp.int32, (rows, pair_w), 1)
    first_half = lax.rem(lane, head) < half
    angles = jnp.exp(lax.rem(lane, half).astype(F32) * (-2.0 * math.log(ROPE_BASE) / head)) * pos_col
    cos_t = jnp.cos(angles)
    sin_t = jnp.where(first_half, -jnp.sin(angles), jnp.sin(angles))

    def rotate(u):
        swapped = jnp.where(first_half, pltpu.roll(u, pair_w - half, axis=1), pltpu.roll(u, half, axis=1))
        return u * cos_t + swapped * sin_t

    for p in range(pairs):
        q_rows[pl.ds(p, rows, stride=pairs), :] = rotate(qkv_acc[:, p * pair_w:(p + 1) * pair_w].astype(BF16).astype(F32))
    kv = qkv_acc[:, pairs * pair_w:].astype(BF16).astype(F32)
    kv = jnp.where(lane < head, rotate(kv), kv)
    new_kv[...] = jnp.transpose(jnp.concatenate([kv, jnp.zeros((128 - rows, pair_w), F32)], axis=0)).astype(BF16)

    scale = head ** -0.5
    lane_s = lax.broadcasted_iota(jnp.int32, (2 * head, seq), 1)
    sub_b = lax.broadcasted_iota(jnp.int32, (2 * head, seq), 0)
    lane_h = lax.broadcasted_iota(jnp.int32, (pairs, 2 * head), 1)

    batch = 8

    def attend_body(i, carry):
        bs = [i * batch + k for k in range(batch)]
        at = [pl.ds(pl.multiple_of(b * head, head), head) for b in bs]
        rr = [pl.ds(pl.multiple_of(b * pairs, pairs), pairs) for b in bs]
        k_old = [k_buf[r, :] for r in at]
        v_old = [v_buf[r, :] for r in at]
        q2 = [q_rows[r, :] for r in rr]
        pos = [pos_smem[0, b] for b in bs]
        pick = jnp.concatenate([jnp.where(sub_b == b, 1.0, 0.0).astype(BF16) for b in bs], axis=1)
        col = jnp.dot(new_kv[...], pick, preferred_element_type=F32)
        keys, vals, scores = [], [], []
        for k in range(batch):
            here = lane_s[0:head] == pos[k]
            c = col[:, k * seq:(k + 1) * seq]
            keys.append(jnp.where(here, c[0:head], k_old[k].astype(F32)).astype(BF16))
            vals.append(jnp.where(here, c[head:], v_old[k].astype(F32)).astype(BF16))
        for k in range(batch):
            q = jnp.concatenate([jnp.where(lane_h < head, q2[k], 0.0), jnp.where(lane_h < head, 0.0, q2[k])], axis=0).astype(BF16)
            s = jnp.dot(q, jnp.concatenate([keys[k], keys[k]], axis=0), preferred_element_type=F32) * scale
            scores.append(jnp.where(lane_s[0:2 * pairs] <= pos[k], s, NEG_BIG))
        top = [jnp.max(s, axis=1, keepdims=True) for s in scores]
        e = [jnp.exp(s - m) for s, m in zip(scores, top)]
        den = [jnp.sum(x, axis=1, keepdims=True) for x in e]
        p = [(x / d).astype(BF16) for x, d in zip(e, den)]
        o = [lax.dot_general(p[k], jnp.concatenate([vals[k], vals[k]], axis=0), (((1,), (1,)), ((), ())), preferred_element_type=F32) for k in range(batch)]
        for k in range(batch):
            ctx_rows[rr[k], :] = jnp.where(lane_h < head, o[k][0:pairs], o[k][pairs:])
        for k in range(batch):
            k_buf[at[k], :] = keys[k]
            v_buf[at[k], :] = vals[k]
        return carry

    with jax.named_scope('attend'):
        lax.fori_loop(0, rows // batch, attend_body, 0)
    for p in range(pairs):
        act[:, CHUNK + ff + p * 2 * head: CHUNK + ff + (p + 1) * 2 * head] = ctx_rows[pl.ds(p, rows, stride=pairs), :].astype(BF16)

    pre[...] = jnp.zeros_like(pre)

    def up_body(n, carry):
        @pl.when((n > 0) & (n + A_SLOTS - 1 < n_up))
        def _():
            start_up(n + A_SLOTS - 1)

        @pl.when(n + A_SLOTS - 1 == n_up)
        def _():
            for c in range(1, B_SLOTS):
                start_down(c)

        @pl.when(n + A_SLOTS - 1 >= n_up)
        def _():
            start_down(n + A_SLOTS - 1 - n_up + B_SLOTS)

        with jax.named_scope('up_wait'):
            wait_up(n)
        act[:, pl.ds(pl.multiple_of(n * CHUNK, CHUNK), CHUNK)] = gelu_exact(pre[...]).astype(BF16)
        pre[...] = jnp.dot(mlp_in[...], ring[pl.ds(pl.multiple_of(a_slot(n) * width, width), width), :], preferred_element_type=F32)
        return carry

    with jax.named_scope('up'):
        lax.fori_loop(0, n_up, up_body, 0)
    act[:, ff:ff + CHUNK] = gelu_exact(pre[...]).astype(BF16)

    n_paired = n_down - N_DIRECT

    far_first = sorted(range(1, n_tp), key=lambda d: -min(d // 2, n_chips - d // 2))

    def peer(d):
        return lax.rem(chip + d // 2, n_chips) * 2 + lax.rem(core + d % 2, 2)

    my_rows = pl.ds(pl.multiple_of(core * half_rows, half_rows), half_rows)
    other_rows = pl.ds(pl.multiple_of((1 - core) * half_rows, half_rows), half_rows)

    def chunk_cols(c):
        return pl.ds(pl.multiple_of(c * CHUNK, CHUNK), CHUNK)

    def quarter_cols(c, q):
        return pl.ds(pl.multiple_of(c * CHUNK + q * quarter, quarter), quarter)

    def slot_cols(c):
        return pl.ds(pl.multiple_of(c * quarter, quarter), quarter)

    def send_pair(c):
        pltpu.make_async_remote_copy(src_ref=part_buf.at[other_rows, chunk_cols(c)], dst_ref=pair_in.at[:, chunk_cols(c)],
                                     send_sem=sem_sent.at[0], recv_sem=sem_pair.at[lax.rem(c, PAIR_SEMS)],
                                     device_id={'tp': chip * 2 + 1 - core}, device_id_type=pl.DeviceIdType.MESH).start()

    def send_quarters(c):
        pltpu.make_async_copy(pair_in.at[:, chunk_cols(c)], pair_in.at[:, chunk_cols(c)], sem_pair.at[lax.rem(c, PAIR_SEMS)]).wait()
        both = part_buf[my_rows, chunk_cols(c)].astype(F32) + pair_in[:, chunk_cols(c)].astype(F32)
        sum_buf[:, chunk_cols(c)] = both.astype(BF16)
        for d in sorted(range(1, n_chips), key=lambda d: -min(d, n_chips - d)):
            q = lax.rem(chip + d, n_chips)
            pltpu.make_async_remote_copy(src_ref=sum_buf.at[:, quarter_cols(c, q)], dst_ref=quarter_in.at[d - 1, :, slot_cols(c)],
                                         send_sem=sem_sent.at[0], recv_sem=sem_quarter.at[lax.rem(c, QUARTER_SEMS)],
                                         device_id={'tp': q * 2 + core}, device_id_type=pl.DeviceIdType.MESH).start()

    def send_result(c):
        total = x_buf[my_rows, quarter_cols(c, chip)].astype(F32) + sum_buf[:, quarter_cols(c, chip)].astype(F32)
        pltpu.make_async_copy(quarter_in.at[:, :, slot_cols(c)], quarter_in.at[:, :, slot_cols(c)], sem_quarter.at[lax.rem(c, QUARTER_SEMS)]).wait()
        for d in range(1, n_chips):
            total = total + quarter_in[d - 1, :, slot_cols(c)].astype(F32)
        gather(c, total)

    def gather(c, total):
        out_buf[my_rows, quarter_cols(c, chip)] = total.astype(BF16)
        for d in far_first:
            pltpu.make_async_remote_copy(src_ref=out_buf.at[my_rows, quarter_cols(c, chip)], dst_ref=out_buf.at[my_rows, quarter_cols(c, chip)],
                                         send_sem=sem_sent.at[0], recv_sem=sem_gather.at[0],
                                         device_id={'tp': peer(d)}, device_id_type=pl.DeviceIdType.MESH).start()

    def send_direct(c):
        for d in far_first:
            to = peer(d)
            src = part_buf.at[pl.ds(pl.multiple_of(lax.rem(to, 2) * half_rows, half_rows), half_rows), quarter_cols(c, to // 2)]
            pltpu.make_async_remote_copy(src_ref=src, dst_ref=last_in.at[c - n_paired, d - 1], send_sem=sem_sent.at[0], recv_sem=sem_last.at[c - n_paired],
                                         device_id={'tp': to}, device_id_type=pl.DeviceIdType.MESH).start()

    def send_result_direct(c):
        total = x_buf[my_rows, quarter_cols(c, chip)].astype(F32) + part_buf[my_rows, quarter_cols(c, chip)].astype(F32)
        pltpu.make_async_copy(last_in.at[c - n_paired], last_in.at[c - n_paired], sem_last.at[c - n_paired]).wait()
        for d in range(1, n_tp):
            total = total + last_in[c - n_paired, d - 1].astype(F32)
        gather(c, total)

    lag = 4
    pl.semaphore_wait(barrier, n_tp - 1)
    start_down(n_slots - 1)

    def multiply(c, groups):
        total = None
        for span in groups:
            with jax.named_scope('down_wait'):
                for i in span:
                    down_copy(c, i, sem_b.at[n_slots + i] if len(groups) > 1 else sem_b.at[lax.rem(c, n_slots)]).wait()
            first, count = parts[span[0]][0], sum(parts[i][1] for i in span)
            w = ring[pl.ds(down_base(c) + first, count), :]
            d = jnp.dot(act[:, CHUNK + first:CHUNK + first + count], w, preferred_element_type=F32)
            total = d if total is None else total + d
        part_buf[:, chunk_cols(c)] = total.astype(BF16)

    def down_body(c, carry):
        @pl.when((c > 0) & (c + n_slots < n_down))
        def _():
            start_down(c + n_slots - 1)

        @pl.when(c + n_slots == n_down)
        def _():
            start_last_down()

        multiply(c, ((0, 1, 2),))
        send_pair(c)

        @pl.when(c >= 1)
        def _():
            with jax.named_scope('quarters'):
                send_quarters(c - 1)

        @pl.when(c >= lag)
        def _():
            with jax.named_scope('result'):
                send_result(c - lag)

        return carry

    with jax.named_scope('down'):
        lax.fori_loop(0, n_paired, down_body, 0)
    done = n_paired - lag
    for c in range(n_paired, n_down):
        with jax.named_scope('tail_multiply'):
            multiply(c, ((0, 1, 2),) if c < n_down - 1 else ((0,), (1,), (2,)))
        send_direct(c)
        if c == n_paired:
            with jax.named_scope('tail_quarters'):
                send_quarters(c - 1)
        with jax.named_scope('tail_result'):
            send_result(done)
        done += 1
    for c in range(done, n_paired):
        with jax.named_scope('tail_result'):
            send_result(c)
    for c in range(n_paired, n_down):
        with jax.named_scope('tail_direct'):
            send_result_direct(c)

    def settle(sem, n_rows):
        pltpu.make_async_copy(out_buf.at[0:n_rows, :], out_buf.at[0:n_rows, :], sem).wait()

    with jax.named_scope('gather_wait'):
        settle(sem_gather.at[0], (n_tp - 1) * rows // n_tp)
    with jax.named_scope('sent_wait'):
        sent = pltpu.make_async_copy(part_buf.at[other_rows, 0:n_paired * CHUNK], part_buf.at[other_rows, 0:n_paired * CHUNK], sem_sent.at[0])
        sent.wait()
        for d in range(1, n_chips):
            pltpu.make_async_copy(quarter_in.at[d - 1, :, 0:n_paired * quarter], quarter_in.at[d - 1, :, 0:n_paired * quarter], sem_sent.at[0]).wait()
        settle(sem_sent.at[0], (n_tp - 1) * rows // n_tp)
        pltpu.make_async_copy(last_in, last_in, sem_sent.at[0]).wait()


def write_kernel(a_ref, b_ref, c_ref, a_out, b_out, c_out, sem):
    copies = []
    for i, (src, dst) in enumerate(((a_ref, a_out), (b_ref, b_out), (c_ref, c_out))):
        copies.append(pltpu.make_async_copy(src, dst, sem.at[i]))
    for c in copies:
        c.start()
    for c in copies:
        c.wait()


def solution(mesh):
    row_spec = P('dp', None)
    vec_spec = P(None)
    cache_spec = P('dp', 'tp', None, None)

    def device_step(x, ga, ba, gm, bm, w_qkv, w_out, w_up, w_down, k_cache, v_cache, positions):
        rows, width = x.shape
        ff = w_up.shape[1]
        n_query, head = w_qkv.shape[2] - 2, w_qkv.shape[3]
        seq = k_cache.shape[2]
        ctx_w = n_query * head
        qk_rows = (n_query + 2) * head
        n_qkv = width // CHUNK
        n_tp = mesh.shape['tp']
        n_chips = n_tp // 2
        n_down = width // CHUNK
        dims = (rows, width, ff, n_query, head, seq, n_tp)
        wq = jnp.transpose(w_qkv, (1, 2, 3, 0)).reshape(qk_rows, width)
        wo = w_out.reshape(ctx_w, width)
        kt = jnp.transpose(k_cache, (0, 1, 3, 2)).reshape(rows * head, seq)
        vt = jnp.transpose(v_cache, (0, 1, 3, 2)).reshape(rows * head, seq)
        any_spec = pl.BlockSpec(memory_space=pl.ANY)
        vmem_spec = pl.BlockSpec(memory_space=pltpu.VMEM)
        out, k_new, v_new = pl.pallas_call(
            lambda *refs: layer_kernel(dims, *refs),
            name='layer',
            out_shape=(pltpu.VMEM((rows, width), BF16), pltpu.VMEM(kt.shape, BF16), pltpu.VMEM(vt.shape, BF16)),
            in_specs=[any_spec] * 12,
            out_specs=(vmem_spec, vmem_spec, vmem_spec),
            scratch_shapes=[
                pltpu.VMEM((A_SLOTS * width + B_SLOTS * (ff + ctx_w), CHUNK), BF16),
                pltpu.VMEM((rows, width), BF16),
                pltpu.VMEM((rows, width), BF16),
                pltpu.VMEM((rows, width), BF16),
                pltpu.VMEM((rows, CHUNK + ff + ctx_w), BF16),
                pltpu.VMEM((rows, qk_rows), F32),
                pltpu.VMEM((2 * head, 128), BF16),
                pltpu.VMEM((rows * n_query // 2, 128), F32),
                pltpu.VMEM((rows * n_query // 2, 128), F32),
                pltpu.VMEM((rows, CHUNK), F32),
                pltpu.VMEM((4, width), F32),
                pltpu.VMEM((1, rows), jnp.int32),
                pltpu.SMEM((1, rows), jnp.int32),
                pltpu.VMEM((rows, width), BF16),
                pltpu.VMEM((rows // 2, width), BF16),
                pltpu.VMEM((rows // 2, width), BF16),
                pltpu.VMEM((n_chips - 1, rows // 2, width // n_chips), BF16),
                pltpu.VMEM((N_DIRECT, n_tp - 1, rows // 2, CHUNK // n_chips), BF16),
                pltpu.SemaphoreType.DMA((2,)),
                pltpu.SemaphoreType.DMA((n_qkv // QKV_GROUP,)),
                pltpu.SemaphoreType.DMA((A_SLOTS,)),
                pltpu.SemaphoreType.DMA((A_SLOTS + B_SLOTS + 3,)),
                pltpu.SemaphoreType.DMA((PAIR_SEMS,)),
                pltpu.SemaphoreType.DMA((QUARTER_SEMS,)),
                pltpu.SemaphoreType.DMA((1,)),
                pltpu.SemaphoreType.DMA((N_DIRECT,)),
                pltpu.SemaphoreType.DMA((1,)),
            ],
            compiler_params=pltpu.CompilerParams(vmem_limit_bytes=60 * 1024 * 1024, collective_id=0, has_side_effects=True),
        )(x, ga.reshape(1, width), ba.reshape(1, width), gm.reshape(1, width), bm.reshape(1, width), wq, wo, w_up, w_down, kt, vt, positions.reshape(1, rows))
        out, k_new, v_new = (pltpu.with_memory_space_constraint(v, pltpu.VMEM) for v in (out, k_new, v_new))
        out, k_new, v_new = pl.pallas_call(
            write_kernel,
            name='write',
            out_shape=(jax.ShapeDtypeStruct((rows, width), BF16), jax.ShapeDtypeStruct(kt.shape, BF16), jax.ShapeDtypeStruct(vt.shape, BF16)),
            in_specs=[vmem_spec] * 3,
            out_specs=(any_spec, any_spec, any_spec),
            scratch_shapes=[pltpu.SemaphoreType.DMA((3,))],
            compiler_params=pltpu.CompilerParams(vmem_limit_bytes=1024 * 1024),
        )(out, k_new, v_new)
        k_new = jnp.transpose(k_new.reshape(rows, 1, head, seq), (0, 1, 3, 2))
        v_new = jnp.transpose(v_new.reshape(rows, 1, head, seq), (0, 1, 3, 2))
        return out, k_new, v_new

    return jax.shard_map(device_step, mesh=mesh, in_specs=(row_spec, vec_spec, vec_spec, vec_spec, vec_spec, P(None, 'tp', None, None), P('tp', None, None, None), P(None, 'tp'), P('tp', None), cache_spec, cache_spec, P('dp')), out_specs=(row_spec, cache_spec, cache_spec), check_vma=False)
```
